512 devices in a mesh: owner: 64 (over z_hi, y, core), rows: 8 (over z_lo, x).
Axes of the slice: x: 4, y: 4, z: 16 (z_hi: 8, z_lo: 2; z = z_hi * 2 + z_lo), core: 2. Of those that a mesh axis runs over, the one named last changes fastest.
Arguments:
- w_gate: float32 [64, 2048, 1024], P('owner', 'rows'), may hold values from -0.1875 to 0.1875
- avg_gate: float32 [64, 2048, 1024], P('owner', 'rows'), may hold values from -0.125 to 0.125
- w_up: float32 [64, 2048, 1024], P('owner', 'rows'), may hold values from -0.1875 to 0.1875
- avg_up: float32 [64, 2048, 1024], P('owner', 'rows'), may hold values from -0.125 to 0.125
- mix_share: float32 [64], P('owner'), may hold values from 0.2 to 0.8
- router_weight: float32 [2048, 64], P('rows', 'owner'), may hold values from -0.125 to 0.125
- router_gain: float32 [2048], P('rows'), may hold values from 0.25 to 1.75
Outputs:
- serve_gate: bfloat16 [64, 2048, 1024], P('owner')
- serve_up: bfloat16 [64, 2048, 1024], P('owner')
- scale_gate: float32 [64, 1024], P('owner')
- scale_up: float32 [64, 1024], P('owner')
- serve_router: bfloat16 [2048, 64], replicated
The draws below stay inside these ranges and needn't reach their ends.
All inputs are finite; a program needn't handle non-finite values.
Results may differ from the reference program's by a relative error of at most 0.0015.
Values may be sent and summed in bfloat16 or wider, within the bound.
A program may use at most 64 MiB of HBM per device.

```python
import jax
import jax.numpy as jnp
from jax import lax

EXPERTS = 64
D_MODEL = 2048
D_EXPERT = 1024


def raised(drawn, own_key, source, target, blocks, factor):
    def block_of(axis_at):
        return (jnp.arange(drawn.shape[axis_at]) // (drawn.shape[axis_at] // blocks)).reshape((-1,) + (1,) * (drawn.ndim - 1 - axis_at))

    near = jax.random.permutation(own_key, blocks)[block_of(target)]
    far = (block_of(target) + blocks // 2) % blocks
    return jnp.where((block_of(source) == near) | (block_of(source) == far), factor * drawn, drawn)


def level_of(key, shape, pieces, least, largest):
    factor_of = 1.0
    for position, blocks in pieces:
        heights = jax.random.uniform(jax.random.fold_in(jax.random.fold_in(key, 6), position), (blocks,), jnp.float32, least / len(pieces), largest / len(pieces))
        factor_of = factor_of * jnp.repeat(jnp.exp(heights), shape[position] // blocks).reshape((-1,) + (1,) * (len(shape) - 1 - position))
    return factor_of


def scatter_about(key, dims, width, most, cuts=(), held_as=jnp.bfloat16):
    drawn = jax.random.normal(key, dims, jnp.float32) * width
    if len(cuts) > 0:
        drawn = level_of(key, dims, cuts, -0.22, 0.18) * drawn
    return jnp.clip(drawn, min=-most, max=most).astype(held_as)


def heavy_noise(own_key, shape, spread, reach, split, heavy, kind=jnp.bfloat16):
    values = spread * jax.random.normal(own_key, shape, jnp.float32)
    if split:
        values = values * level_of(own_key, shape, split, -0.22, 0.18)
    return jnp.clip(raised(values, jax.random.fold_in(own_key, 3), *heavy), -reach, reach).astype(kind)


def setup_inputs(seed: int = 0) -> dict:
    key_of = jax.random.split(jax.random.key(seed), 8)
    w_gate = heavy_noise(key_of[0], (EXPERTS, D_MODEL, D_EXPERT), D_MODEL ** -0.5, 0.1875, ((0, 64), (1, 8)), (1, 2, 8, 2.0), jnp.float32)
    avg_gate = scatter_about(key_of[1], (EXPERTS, D_MODEL, D_EXPERT), D_MODEL ** -0.5, 0.125, ((0, 64), (1, 8)), jnp.float32)
    w_up = heavy_noise(key_of[2], (EXPERTS, D_MODEL, D_EXPERT), D_MODEL ** -0.5, 0.1875, ((0, 64), (1, 8)), (1, 2, 8, 2.0), jnp.float32)
    avg_up = scatter_about(key_of[3], (EXPERTS, D_MODEL, D_EXPERT), D_MODEL ** -0.5, 0.125, ((0, 64), (1, 8)), jnp.float32)
    mix_share = jnp.clip(0.2 + 0.6 * jax.random.uniform(key_of[4], (EXPERTS,), jnp.float32) ** level_of(key_of[4], (EXPERTS,), ((0, 64),), -0.2, 0.2), 0.2, 0.8)
    router_weight = scatter_about(key_of[5], (D_MODEL, EXPERTS), D_MODEL ** -0.5, 0.125, ((0, 8), (1, 64)), jnp.float32)
    router_gain = jnp.clip(1.0 + 0.15 * jax.random.normal(key_of[6], (D_MODEL,), jnp.float32), 0.25, 1.75)
    return {"w_gate": w_gate, "avg_gate": avg_gate, "w_up": w_up, "avg_up": avg_up, "mix_share": mix_share, "router_weight": router_weight, "router_gain": router_gain}


def reference(w_gate, avg_gate, w_up, avg_up, mix_share, router_weight, router_gain):
    fresh_gate = mix_share[:, None, None] * w_gate + (1.0 - mix_share[:, None, None]) * avg_gate
    fresh_up = mix_share[:, None, None] * w_up + (1.0 - mix_share[:, None, None]) * avg_up
    scale_gate = jnp.sqrt(lax.optimization_barrier(jnp.sum(fresh_gate * fresh_gate, axis=1)))
    serve_gate = (fresh_gate / jnp.expand_dims(scale_gate, 1)).astype(jnp.bfloat16)
    scale_up = jnp.sqrt(lax.optimization_barrier(jnp.sum(fresh_up * fresh_up, axis=1)))
    serve_up = (fresh_up / jnp.expand_dims(scale_up, 1)).astype(jnp.bfloat16)
    serve_router = (router_weight * router_gain[:, None]).astype(jnp.bfloat16)
    return (serve_gate, serve_up, scale_gate, scale_up, serve_router)
```

```python
import functools

import jax
import jax.numpy as jnp
from jax import lax
from jax.experimental import pallas as pl
from jax.experimental.pallas import tpu as pltpu
from jax.sharding import PartitionSpec as P

SIDE = 4
STEP = 16
ACROSS = 9


def chunk_at(k, first):
    held = ACROSS if first else 16 - ACROSS
    return k // held, k % held + (0 if first else ACROSS)


def gather_kernel(mix, w_gate, avg_gate, w_up, avg_up, out, scale, fresh, other, stats, load, sent, stat_sent, stat_got, got):
    me = lax.axis_index("rows")
    x, z = me % SIDE, me // SIDE
    right, left = z * SIDE + (x + 1) % SIDE, z * SIDE + (x + SIDE - 1) % SIDE
    across = (1 - z) * SIDE + x
    far = z * SIDE + (x + 2) % SIDE
    share = fresh.shape[1]
    n_first, n_rest = 2 * ACROSS, 2 * (16 - ACROSS)

    loads = []
    for i, (source, target) in enumerate(
        ((w_gate, fresh.at[0]), (avg_gate, other.at[0]), (w_up, fresh.at[1]), (avg_up, other.at[1]))
    ):
        loads.append(pltpu.make_async_copy(source.at[0], target, load.at[i]))
        loads[-1].start()

    barrier = pltpu.get_barrier_semaphore()
    for hop in range(1, 2 * SIDE):
        pl.semaphore_signal(barrier, inc=1, device_id={"rows": (me + hop) % (2 * SIDE)}, device_id_type=pl.DeviceIdType.MESH)

    part = mix[0]
    for a in range(2):
        loads[2 * a].wait()
        loads[2 * a + 1].wait()

        def mixed(i, total):
            rows = pl.ds(pl.multiple_of(i * 8, 8), 8)
            value = part * fresh[a, rows, :] + (1.0 - part) * other[a, rows, :]
            fresh[a, rows, :] = value
            return total + value * value

        total = lax.fori_loop(0, share // 8, mixed, jnp.zeros((8, fresh.shape[2]), jnp.float32), unroll=4)
        stats[me, pl.ds(a, 1), :] = jnp.sum(total, axis=0, keepdims=True)

    pl.semaphore_wait(barrier, 2 * SIDE - 1)

    def stat_copy(hop):
        return pltpu.make_async_remote_copy(
            src_ref=stats.at[me],
            dst_ref=stats.at[me],
            send_sem=stat_sent.at[hop],
            recv_sem=stat_got.at[me],
            device_id={"rows": (me + hop) % (2 * SIDE)},
            device_id_type=pl.DeviceIdType.MESH,
        )

    for hop in range(1, 2 * SIDE):
        stat_copy(hop).start()
    for hop in range(1, 2 * SIDE):
        source = (me + hop) % (2 * SIDE)
        pltpu.make_async_copy(stats.at[source], stats.at[source], stat_got.at[source]).wait()
    total = stats[0]
    for source in range(1, 2 * SIDE):
        total = total + stats[source]
    scale[...] = jnp.sqrt(total)

    def place(source, a, i):
        return out.at[a, pl.ds(pl.multiple_of(source * share + i * STEP, STEP), STEP), :]

    def send(source, a, i, target, link):
        pltpu.make_async_remote_copy(
            src_ref=place(source, a, i),
            dst_ref=place(source, a, i),
            send_sem=sent.at[link],
            recv_sem=got.at[source, a * 16 + i],
            device_id={"rows": target},
            device_id_type=pl.DeviceIdType.MESH,
        ).start()

    def arrived(source, a, i):
        pltpu.make_async_copy(place(source, a, i), place(source, a, i), got.at[source, a * 16 + i]).wait()

    def settle(a, i):
        rows = pl.ds(pl.multiple_of(i * STEP, STEP), STEP)
        value = fresh[a, rows, :] / scale[pl.ds(a, 1), :]
        out[a, pl.ds(pl.multiple_of(me * share + i * STEP, STEP), STEP), :] = value.astype(jnp.bfloat16)

    def own_step(k, _):
        @pl.when(k < n_first)
        def _():
            settle(*chunk_at(k, True))

        @pl.when(k < n_rest)
        def _():
            settle(*chunk_at(k, False))

        @pl.when(k > 0)
        def _():
            a, i = chunk_at(k - 1, True)
            send(me, a, i, across, 2)

        @pl.when((k > 0) & (k <= n_rest))
        def _():
            a, i = chunk_at(k - 1, False)
            send(me, a, i, right, 0)
            send(me, a, i, left, 1)

        return 0

    lax.fori_loop(0, n_first + 1, own_step, 0)

    def own_next(k, _):
        a, i = chunk_at(k, True)
        send(me, a, i, right, 0)
        send(me, a, i, left, 1)

        @pl.when(k < n_rest)
        def _():
            a, i = chunk_at(k, False)
            send(me, a, i, across, 2)

        return 0

    lax.fori_loop(0, n_first, own_next, 0)

    def near(k, first, z_too, from_left, from_right):
        a, i = chunk_at(k, first)
        arrived(from_left, a, i)
        arrived(from_right, a, i)
        if z_too:
            send(from_left, a, i, across, 2)
            send(from_right, a, i, across, 2)

        @pl.when(k % 2 == 0)
        def _():
            send(from_left, a, i, right, 0)

        @pl.when(k % 2 == 1)
        def _():
            send(from_right, a, i, left, 1)

        return 0

    lax.fori_loop(0, n_rest, lambda k, _: near(k, False, True, left, right), 0)

    def from_across(k, _):
        a, i = chunk_at(k, True)
        arrived(across, a, i)
        send(across, a, i, right, 0)
        send(across, a, i, left, 1)
        return 0

    lax.fori_loop(0, n_first, from_across, 0)
    lax.fori_loop(0, n_first, lambda k, _: near(k, True, False, left, right), 0)

    def far_rest(k, _):
        a, i = chunk_at(k, False)
        arrived(far, a, i)
        send(far, a, i, across, 2)
        return 0

    lax.fori_loop(0, n_rest, far_rest, 0)

    def flip(r):
        return (r + SIDE) % (2 * SIDE)

    lax.fori_loop(0, n_first, lambda k, _: near(k, True, False, flip(left), flip(right)), 0)

    def last_first(k, _):
        a, i = chunk_at(k, True)
        arrived(far, a, i)
        arrived(flip(far), a, i)
        return 0

    lax.fori_loop(0, n_first, last_first, 0)

    def last_rest(k, _):
        a, i = chunk_at(k, False)
        for source in (across, flip(left), flip(right), flip(far)):
            arrived(source, a, i)
        return 0

    lax.fori_loop(0, n_rest, last_rest, 0)

    for hop in range(1, 2 * SIDE):
        stat_copy(hop).wait_send()
    on_x = (n_rest + n_first) + n_rest // 2 + n_first + n_first // 2 + n_first // 2
    on_z = n_first + n_rest + 3 * n_rest
    for link, count in ((0, on_x), (1, on_x), (2, on_z)):
        all_sent = out.at[0, pl.ds(0, count * STEP), :]
        pltpu.make_async_copy(all_sent, all_sent, sent.at[link]).wait()


def place_kernel(gathered, scale, serve_gate, serve_up, scale_gate, scale_up, done):
    copies = (
        pltpu.make_async_copy(gathered.at[pl.ds(0, 1)], serve_gate, done.at[0]),
        pltpu.make_async_copy(gathered.at[pl.ds(1, 1)], serve_up, done.at[1]),
        pltpu.make_async_copy(scale.at[pl.ds(0, 1)], scale_gate, done.at[2]),
        pltpu.make_async_copy(scale.at[pl.ds(1, 1)], scale_up, done.at[3]),
    )
    for copy in copies:
        copy.start()
    for copy in copies:
        copy.wait()


def shards(w_gate, avg_gate, w_up, avg_up, mix_share, router_weight, router_gain):
    _, share, width = w_gate.shape
    n = lax.axis_size("rows")
    in_hbm = pl.BlockSpec(memory_space=pltpu.HBM)
    in_vmem = pl.BlockSpec(memory_space=pltpu.VMEM)
    gathered, scale = pl.pallas_call(
        gather_kernel,
        out_shape=(
            jax.ShapeDtypeStruct((2, n * share, width), jnp.bfloat16),
            jax.ShapeDtypeStruct((2, width), jnp.float32),
        ),
        in_specs=[pl.BlockSpec(memory_space=pltpu.SMEM)] + [in_hbm] * 4,
        out_specs=(in_vmem, in_vmem),
        scratch_shapes=[
            pltpu.VMEM((2, share, width), jnp.float32),
            pltpu.VMEM((2, share, width), jnp.float32),
            pltpu.VMEM((n, 2, width), jnp.float32),
            pltpu.SemaphoreType.DMA((4,)),
            pltpu.SemaphoreType.DMA((3,)),
            pltpu.SemaphoreType.DMA((n,)),
            pltpu.SemaphoreType.DMA((n,)),
            pltpu.SemaphoreType.DMA((n, 32)),
        ],
        compiler_params=pltpu.CompilerParams(collective_id=0, has_side_effects=True, vmem_limit_bytes=32 * 2**20),
        name="gather",
    )(mix_share, *(pltpu.with_memory_space_constraint(w, pltpu.HBM) for w in (w_gate, avg_gate, w_up, avg_up)))
    serve_gate, serve_up, scale_gate, scale_up = pl.pallas_call(
        place_kernel,
        out_shape=(
            jax.ShapeDtypeStruct((1, n * share, width), jnp.bfloat16),
            jax.ShapeDtypeStruct((1, n * share, width), jnp.bfloat16),
            jax.ShapeDtypeStruct((1, width), jnp.float32),
            jax.ShapeDtypeStruct((1, width), jnp.float32),
        ),
        in_specs=[in_vmem, in_vmem],
        out_specs=(in_hbm,) * 4,
        scratch_shapes=[pltpu.SemaphoreType.DMA((4,))],
        compiler_params=pltpu.CompilerParams(vmem_limit_bytes=32 * 2**20),
        name="place",
    )(gathered, scale)
    part_router = (router_weight * router_gain[:, None]).astype(jnp.bfloat16)
    row_router = lax.all_gather(part_router, "rows", axis=0, tiled=True)
    serve_router = lax.all_gather(row_router, "owner", axis=1, tiled=True)
    return (serve_gate, serve_up, scale_gate, scale_up, serve_router)


def solution(mesh):
    placed = (
        P("owner", "rows", None),
        P("owner", "rows", None),
        P("owner", "rows", None),
        P("owner", "rows", None),
        P("owner"),
        P("rows", "owner"),
        P("rows"),
    )
    return jax.shard_map(
        shards,
        mesh=mesh,
        in_specs=placed,
        out_specs=(
            P("owner", None, None),
            P("owner", None, None),
            P("owner", None),
            P("owner", None),
            P(),
        ),
        check_vma=False,
    )
```

```python
import functools

import jax
import jax.numpy as jnp
from jax import lax
from jax.experimental import pallas as pl
from jax.experimental.pallas import tpu as pltpu
from jax.sharding import PartitionSpec as P

SIDE = 4
STEP = 16
TALL, WIDE, CORES = 8, 4, 2
ACROSS = 9


def chunk_at(k, first):
    held = ACROSS if first else 16 - ACROSS
    return k // held, k % held + (0 if first else ACROSS)


def gather_kernel(
    mix, w_gate, avg_gate, w_up, avg_up, weight, gain,
    out, scale, router,
    fresh, other, stats, line, land, block,
    load, sent, stat_sent, stat_got, got,
    line_sent, line_got, ring_sent, ring_got, wide_sent, wide_got, core_sent, core_got,
):
    me = lax.axis_index("rows")
    owner = lax.axis_index("owner")
    high, y, core = owner // (WIDE * CORES), owner // CORES % WIDE, owner % CORES
    x, z = me % SIDE, me // SIDE
    right, left = z * SIDE + (x + 1) % SIDE, z * SIDE + (x + SIDE - 1) % SIDE
    across = (1 - z) * SIDE + x
    far = z * SIDE + (x + 2) % SIDE
    share = fresh.shape[1]
    n_first, n_rest = 2 * ACROSS, 2 * (16 - ACROSS)

    def at_owner(h, j, c):
        return {"owner": (h * WIDE + j) * CORES + c}

    loads = []
    for i, (source, target) in enumerate(
        (
            (w_gate.at[0], fresh.at[0]),
            (avg_gate.at[0], other.at[0]),
            (w_up.at[0], fresh.at[1]),
            (avg_up.at[0], other.at[1]),
            (weight, line.at[0]),
            (gain, line.at[1]),
        )
    ):
        loads.append(pltpu.make_async_copy(source, target, load.at[i]))
        loads[-1].start()

    barrier = pltpu.get_barrier_semaphore()
    for hop in range(1, 2 * SIDE):
        pl.semaphore_signal(barrier, inc=1, device_id={"rows": (me + hop) % (2 * SIDE)}, device_id_type=pl.DeviceIdType.MESH)

    others = [at_owner((high + hop) % TALL, y, core) for hop in (1, TALL - 1)]
    others += [at_owner(high, (y + hop) % WIDE, core) for hop in range(1, WIDE)]
    others.append(at_owner(high, y, 1 - core))
    for target in others:
        pl.semaphore_signal(barrier, inc=1, device_id=target, device_id_type=pl.DeviceIdType.MESH)

    part = mix[0]
    for a in range(2):
        loads[2 * a].wait()
        loads[2 * a + 1].wait()

        def mixed(i, total):
            rows = pl.ds(pl.multiple_of(i * 8, 8), 8)
            value = part * fresh[a, rows, :] + (1.0 - part) * other[a, rows, :]
            fresh[a, rows, :] = value
            return total + value * value

        total = lax.fori_loop(0, share // 8, mixed, jnp.zeros((8, fresh.shape[2]), jnp.float32), unroll=4)
        stats[me, pl.ds(a, 1), :] = jnp.sum(total, axis=0, keepdims=True)

    loads[4].wait()
    loads[5].wait()
    lanes = pl.ds(pl.multiple_of(me * share, share), share)
    land[high, y, core, :, lanes] = (line[0] * line[1]).astype(jnp.bfloat16).astype(jnp.float32)

    pl.semaphore_wait(barrier, 2 * SIDE - 1 + len(others))

    def stat_copy(hop):
        return pltpu.make_async_remote_copy(
            src_ref=stats.at[me],
            dst_ref=stats.at[me],
            send_sem=stat_sent.at[hop],
            recv_sem=stat_got.at[me],
            device_id={"rows": (me + hop) % (2 * SIDE)},
            device_id_type=pl.DeviceIdType.MESH,
        )

    def remote(place, send_sem, recv_sem, target):
        return pltpu.make_async_remote_copy(
            src_ref=place,
            dst_ref=place,
            send_sem=send_sem,
            recv_sem=recv_sem,
            device_id=target,
            device_id_type=pl.DeviceIdType.MESH,
        )

    def line_place(source):
        return land.at[high, y, core, :, pl.ds(pl.multiple_of(source * share, share), share)]

    def line_copy(hop):
        return remote(line_place(me), line_sent.at[hop], line_got.at[me], {"rows": (me + hop) % (2 * SIDE)})

    def ring_copy(way, step):
        towards = 1 if way == 0 else TALL - 1
        tile = (high + (TALL - towards) * step) % TALL
        target = at_owner((high + towards) % TALL, y, core)
        return remote(land.at[tile, y, core], ring_sent.at[way, step], ring_got.at[way, step], target)

    def ring_wait(way, step):
        towards = 1 if way == 0 else TALL - 1
        tile = land.at[(high + (TALL - towards) * (step + 1)) % TALL, y, core]
        pltpu.make_async_copy(tile, tile, ring_got.at[way, step]).wait()

    steps = (TALL // 2, (TALL - 1) // 2)

    def ring_step(step):
        for way in range(2):
            if 0 < step <= steps[way]:
                ring_wait(way, step - 1)
            if step < steps[way]:
                ring_copy(way, step).start()

    def wide_copy(hop):
        target = at_owner(high, (y + hop) % WIDE, core)
        return remote(land.at[:, y, core], wide_sent.at[hop], wide_got.at[y], target)

    def core_copy():
        return remote(land.at[:, :, core], core_sent.at[0], core_got.at[0], at_owner(high, y, 1 - core))

    for hop in range(1, 2 * SIDE):
        stat_copy(hop).start()
    for hop in range(1, 2 * SIDE):
        line_copy(hop).start()
    for hop in range(1, 2 * SIDE):
        source = (me + hop) % (2 * SIDE)
        pltpu.make_async_copy(stats.at[source], stats.at[source], stat_got.at[source]).wait()
    total = stats[0]
    for source in range(1, 2 * SIDE):
        total = total + stats[source]
    scale[...] = jnp.sqrt(total)

    def place(source, a, i):
        return out.at[a, pl.ds(pl.multiple_of(source * share + i * STEP, STEP), STEP), :]

    def send(source, a, i, target, link):
        pltpu.make_async_remote_copy(
            src_ref=place(source, a, i),
            dst_ref=place(source, a, i),
            send_sem=sent.at[link],
            recv_sem=got.at[source, a * 16 + i],
            device_id={"rows": target},
            device_id_type=pl.DeviceIdType.MESH,
        ).start()

    def arrived(source, a, i):
        pltpu.make_async_copy(place(source, a, i), place(source, a, i), got.at[source, a * 16 + i]).wait()

    def settle(a, i):
        rows = pl.ds(pl.multiple_of(i * STEP, STEP), STEP)
        value = fresh[a, rows, :] / scale[pl.ds(a, 1), :]
        out[a, pl.ds(pl.multiple_of(me * share + i * STEP, STEP), STEP), :] = value.astype(jnp.bfloat16)

    paced = (6, 12, 18, 25, 32)

    def own_send(k):
        a, i = chunk_at(k, False) if k < n_rest else chunk_at(k - n_rest, True)
        send(me, a, i, right, 0)
        send(me, a, i, left, 1)
        a, i = chunk_at(k, True) if k < n_first else chunk_at(k - n_first, False)
        send(me, a, i, across, 2)

    for k in range(n_first + 1):
        if k < n_first:
            settle(*chunk_at(k, True))
        if k < n_rest:
            settle(*chunk_at(k, False))
        if 0 < k <= paced[0]:
            own_send(k - 1)

    for hop in range(1, 2 * SIDE):
        source = (me + hop) % (2 * SIDE)
        pltpu.make_async_copy(line_place(source), line_place(source), line_got.at[source]).wait()
    for step in range(len(paced) - 1):
        ring_step(step)
        for k in range(paced[step], paced[step + 1]):
            own_send(k)

    def near(k, first, z_too, from_left, from_right):
        a, i = chunk_at(k, first)
        arrived(from_left, a, i)
        arrived(from_right, a, i)
        if z_too:
            send(from_left, a, i, across, 2)
            send(from_right, a, i, across, 2)

        @pl.when(k % 2 == 0)
        def _():
            send(from_left, a, i, right, 0)

        @pl.when(k % 2 == 1)
        def _():
            send(from_right, a, i, left, 1)

        return 0

    lax.fori_loop(0, n_rest, lambda k, _: near(k, False, True, left, right), 0)

    for step in range(len(paced) - 1, steps[0] + 1):
        ring_step(step)
    for hop in range(1, WIDE):
        wide_copy(hop).start()

    def from_across(k, _):
        a, i = chunk_at(k, True)
        arrived(across, a, i)
        send(across, a, i, right, 0)
        send(across, a, i, left, 1)
        return 0

    lax.fori_loop(0, n_first, from_across, 0)
    lax.fori_loop(0, n_first, lambda k, _: near(k, True, False, left, right), 0)

    for hop in range(1, WIDE):
        source = land.at[:, (y + hop) % WIDE, core]
        pltpu.make_async_copy(source, source, wide_got.at[(y + hop) % WIDE]).wait()
    core_copy().start()

    def far_rest(k, _):
        a, i = chunk_at(k, False)
        arrived(far, a, i)
        send(far, a, i, across, 2)
        return 0

    lax.fori_loop(0, n_rest, far_rest, 0)

    def flip(r):
        return (r + SIDE) % (2 * SIDE)

    lax.fori_loop(0, n_first, lambda k, _: near(k, True, False, flip(left), flip(right)), 0)

    theirs = land.at[:, :, 1 - core]
    pltpu.make_async_copy(theirs, theirs, core_got.at[0]).wait()
    for first in range(0, TALL * WIDE * CORES, 16):

        def line_in(k, _):
            o = first + k
            block[pl.ds(k, 1), :] = land[o // (WIDE * CORES), o // CORES % WIDE, o % CORES]
            return 0

        lax.fori_loop(0, 16, line_in, 0)
        router[pl.ds(first, 16), :] = block[...].astype(jnp.bfloat16)

    def last_first(k, _):
        a, i = chunk_at(k, True)
        arrived(far, a, i)
        arrived(flip(far), a, i)
        return 0

    lax.fori_loop(0, n_first, last_first, 0)

    def last_rest(k, _):
        a, i = chunk_at(k, False)
        for source in (across, flip(left), flip(right), flip(far)):
            arrived(source, a, i)
        return 0

    lax.fori_loop(0, n_rest, last_rest, 0)

    for hop in range(1, 2 * SIDE):
        stat_copy(hop).wait_send()
        line_copy(hop).wait_send()
    for way in range(2):
        for step in range(steps[way]):
            ring_copy(way, step).wait_send()
    for hop in range(1, WIDE):
        wide_copy(hop).wait_send()
    core_copy().wait_send()
    on_x = (n_rest + n_first) + n_rest // 2 + n_first + n_first // 2 + n_first // 2
    on_z = n_first + n_rest + 3 * n_rest
    for link, count in ((0, on_x), (1, on_x), (2, on_z)):
        all_sent = out.at[0, pl.ds(0, count * STEP), :]
        pltpu.make_async_copy(all_sent, all_sent, sent.at[link]).wait()


def place_kernel(gathered, scale, router, serve_gate, serve_up, scale_gate, scale_up, serve_router, done):
    copies = (
        pltpu.make_async_copy(gathered.at[pl.ds(0, 1)], serve_gate, done.at[0]),
        pltpu.make_async_copy(gathered.at[pl.ds(1, 1)], serve_up, done.at[1]),
        pltpu.make_async_copy(scale.at[pl.ds(0, 1)], scale_gate, done.at[2]),
        pltpu.make_async_copy(scale.at[pl.ds(1, 1)], scale_up, done.at[3]),
        pltpu.make_async_copy(router, serve_router, done.at[4]),
    )
    for copy in copies:
        copy.start()
    for copy in copies:
        copy.wait()


def shards(w_gate, avg_gate, w_up, avg_up, mix_share, router_weight, router_gain):
    _, share, width = w_gate.shape
    n = lax.axis_size("rows")
    in_hbm = pl.BlockSpec(memory_space=pltpu.HBM)
    in_vmem = pl.BlockSpec(memory_space=pltpu.VMEM)
    held = (w_gate, avg_gate, w_up, avg_up, router_weight.T, router_gain[None])
    owners = TALL * WIDE * CORES
    gathered, scale, router = pl.pallas_call(
        gather_kernel,
        out_shape=(
            jax.ShapeDtypeStruct((2, n * share, width), jnp.bfloat16),
            jax.ShapeDtypeStruct((2, width), jnp.float32),
            jax.ShapeDtypeStruct((owners, n * share), jnp.bfloat16),
        ),
        in_specs=[pl.BlockSpec(memory_space=pltpu.SMEM)] + [in_hbm] * 6,
        out_specs=(in_vmem,) * 3,
        scratch_shapes=[
            pltpu.VMEM((2, share, width), jnp.float32),
            pltpu.VMEM((2, share, width), jnp.float32),
            pltpu.VMEM((n, 2, width), jnp.float32),
            pltpu.VMEM((2, 1, share), jnp.float32),
            pltpu.VMEM((TALL, WIDE, CORES, 1, n * share), jnp.float32),
            pltpu.VMEM((16, n * share), jnp.float32),
            pltpu.SemaphoreType.DMA((6,)),
            pltpu.SemaphoreType.DMA((3,)),
            pltpu.SemaphoreType.DMA((n,)),
            pltpu.SemaphoreType.DMA((n,)),
            pltpu.SemaphoreType.DMA((n, 32)),
            pltpu.SemaphoreType.DMA((n,)),
            pltpu.SemaphoreType.DMA((n,)),
            pltpu.SemaphoreType.DMA((2, TALL // 2)),
            pltpu.SemaphoreType.DMA((2, TALL // 2)),
            pltpu.SemaphoreType.DMA((WIDE,)),
            pltpu.SemaphoreType.DMA((WIDE,)),
            pltpu.SemaphoreType.DMA((1,)),
            pltpu.SemaphoreType.DMA((1,)),
        ],
        compiler_params=pltpu.CompilerParams(collective_id=0, has_side_effects=True, vmem_limit_bytes=32 * 2**20),
        name="gather",
    )(mix_share, *(pltpu.with_memory_space_constraint(w, pltpu.HBM) for w in held))
    serve_gate, serve_up, scale_gate, scale_up, serve_router = pl.pallas_call(
        place_kernel,
        out_shape=(
            jax.ShapeDtypeStruct((1, n * share, width), jnp.bfloat16),
            jax.ShapeDtypeStruct((1, n * share, width), jnp.bfloat16),
            jax.ShapeDtypeStruct((1, width), jnp.float32),
            jax.ShapeDtypeStruct((1, width), jnp.float32),
            jax.ShapeDtypeStruct((owners, n * share), jnp.bfloat16),
        ),
        in_specs=[in_vmem] * 3,
        out_specs=(in_hbm,) * 5,
        scratch_shapes=[pltpu.SemaphoreType.DMA((5,))],
        compiler_params=pltpu.CompilerParams(vmem_limit_bytes=32 * 2**20),
        name="place",
    )(gathered, scale, router)
    return (serve_gate, serve_up, scale_gate, scale_up, serve_router.T)


def solution(mesh):
    placed = (
        P("owner", "rows", None),
        P("owner", "rows", None),
        P("owner", "rows", None),
        P("owner", "rows", None),
        P("owner"),
        P("rows", "owner"),
        P("rows"),
    )
    return jax.shard_map(
        shards,
        mesh=mesh,
        in_specs=placed,
        out_specs=(
            P("owner", None, None),
            P("owner", None, None),
            P("owner", None),
            P("owner", None),
            P(),
        ),
        check_vma=False,
    )
```

```python
import functools

import jax
import jax.numpy as jnp
from jax import lax
from jax.experimental import pallas as pl
from jax.experimental.pallas import tpu as pltpu
from jax.sharding import PartitionSpec as P

SIDE = 4
STEP = 16
TALL, WIDE, CORES = 8, 4, 2
BEHIND = 8
APART = 11
ACROSS = 9


def chunk_at(k, first):
    held = ACROSS if first else 16 - ACROSS
    return k // held, k % held + (0 if first else ACROSS)


def gather_kernel(
    mix, w_gate, avg_gate, w_up, avg_up, weight, gain,
    out, scale, router,
    fresh, other, stats, line, land, block,
    load, sent, stat_sent, stat_got, got,
    line_sent, line_got, ring_sent, ring_got, wide_sent, wide_got, core_sent, core_got,
):
    me = lax.axis_index("rows")
    owner = lax.axis_index("owner")
    high, y, core = owner // (WIDE * CORES), owner // CORES % WIDE, owner % CORES
    x, z = me % SIDE, me // SIDE
    right, left = z * SIDE + (x + 1) % SIDE, z * SIDE + (x + SIDE - 1) % SIDE
    across = (1 - z) * SIDE + x
    far = z * SIDE + (x + 2) % SIDE
    share = fresh.shape[1]
    n_first, n_rest = 2 * ACROSS, 2 * (16 - ACROSS)

    def at_owner(h, j, c):
        return {"owner": (h * WIDE + j) * CORES + c}

    loads = []
    for i, (source, target) in enumerate(
        (
            (w_gate.at[0], fresh.at[0]),
            (avg_gate.at[0], other.at[0]),
            (w_up.at[0], fresh.at[1]),
            (avg_up.at[0], other.at[1]),
            (weight, line.at[0]),
            (gain, line.at[1]),
        )
    ):
        loads.append(pltpu.make_async_copy(source, target, load.at[i]))
        loads[-1].start()

    barrier = pltpu.get_barrier_semaphore()
    for hop in range(1, 2 * SIDE):
        pl.semaphore_signal(barrier, inc=1, device_id={"rows": (me + hop) % (2 * SIDE)}, device_id_type=pl.DeviceIdType.MESH)

    others = [at_owner((high + hop) % TALL, y, core) for hop in (1, TALL - 1)]
    others += [at_owner(high, (y + hop) % WIDE, core) for hop in range(1, WIDE)]
    others.append(at_owner(high, y, 1 - core))
    for target in others:
        pl.semaphore_signal(barrier, inc=1, device_id=target, device_id_type=pl.DeviceIdType.MESH)

    part = mix[0]
    for a in range(2):
        loads[2 * a].wait()
        loads[2 * a + 1].wait()

        def mixed(i, total):
            rows = pl.ds(pl.multiple_of(i * 8, 8), 8)
            value = part * fresh[a, rows, :] + (1.0 - part) * other[a, rows, :]
            fresh[a, rows, :] = value
            return total + value * value

        total = lax.fori_loop(0, share // 8, mixed, jnp.zeros((8, fresh.shape[2]), jnp.float32), unroll=4)
        stats[me, pl.ds(a, 1), :] = jnp.sum(total, axis=0, keepdims=True)

    loads[4].wait()
    loads[5].wait()
    lanes = pl.ds(pl.multiple_of(me * share, share), share)
    land[high, y, core, :, lanes] = (line[0] * line[1]).astype(jnp.bfloat16).astype(jnp.float32)

    pl.semaphore_wait(barrier, 2 * SIDE - 1 + len(others))

    def stat_copy(hop):
        return pltpu.make_async_remote_copy(
            src_ref=stats.at[me],
            dst_ref=stats.at[me],
            send_sem=stat_sent.at[hop],
            recv_sem=stat_got.at[me],
            device_id={"rows": (me + hop) % (2 * SIDE)},
            device_id_type=pl.DeviceIdType.MESH,
        )

    def remote(place, send_sem, recv_sem, target):
        return pltpu.make_async_remote_copy(
            src_ref=place,
            dst_ref=place,
            send_sem=send_sem,
            recv_sem=recv_sem,
            device_id=target,
            device_id_type=pl.DeviceIdType.MESH,
        )

    def line_place(source):
        return land.at[high, y, core, :, pl.ds(pl.multiple_of(source * share, share), share)]

    def line_copy(hop):
        return remote(line_place(me), line_sent.at[hop], line_got.at[me], {"rows": (me + hop) % (2 * SIDE)})

    def ring_copy(way, step):
        towards = 1 if way == 0 else TALL - 1
        tile = (high + (TALL - towards) * step) % TALL
        target = at_owner((high + towards) % TALL, y, core)
        return remote(land.at[tile, y, core], ring_sent.at[way, step], ring_got.at[way, step], target)

    def ring_wait(way, step):
        towards = 1 if way == 0 else TALL - 1
        tile = land.at[(high + (TALL - towards) * (step + 1)) % TALL, y, core]
        pltpu.make_async_copy(tile, tile, ring_got.at[way, step]).wait()

    steps = (TALL // 2, (TALL - 1) // 2)

    def ring_step(step):
        for way in range(2):
            if 0 < step <= steps[way]:
                ring_wait(way, step - 1)
            if step < steps[way]:
                ring_copy(way, step).start()

    def wide_copy(hop):
        target = at_owner(high, (y + hop) % WIDE, core)
        return remote(land.at[:, y, core], wide_sent.at[hop], wide_got.at[y], target)

    def core_copy():
        return remote(land.at[:, :, core], core_sent.at[0], core_got.at[0], at_owner(high, y, 1 - core))

    for hop in range(1, 2 * SIDE):
        stat_copy(hop).start()
    for hop in range(1, 2 * SIDE):
        line_copy(hop).start()
    for hop in range(1, 2 * SIDE):
        source = (me + hop) % (2 * SIDE)
        pltpu.make_async_copy(stats.at[source], stats.at[source], stat_got.at[source]).wait()
    total = stats[0]
    for source in range(1, 2 * SIDE):
        total = total + stats[source]
    scale[...] = jnp.sqrt(total)

    def place(source, a, i):
        return out.at[a, pl.ds(pl.multiple_of(source * share + i * STEP, STEP), STEP), :]

    def send(source, a, i, target, link):
        pltpu.make_async_remote_copy(
            src_ref=place(source, a, i),
            dst_ref=place(source, a, i),
            send_sem=sent.at[link],
            recv_sem=got.at[source, a * 16 + i],
            device_id={"rows": target},
            device_id_type=pl.DeviceIdType.MESH,
        ).start()

    def arrived(source, a, i):
        pltpu.make_async_copy(place(source, a, i), place(source, a, i), got.at[source, a * 16 + i]).wait()

    def settle(a, i):
        rows = pl.ds(pl.multiple_of(i * STEP, STEP), STEP)
        value = fresh[a, rows, :] / scale[pl.ds(a, 1), :]
        out[a, pl.ds(pl.multiple_of(me * share + i * STEP, STEP), STEP), :] = value.astype(jnp.bfloat16)

    def flip(r):
        return (r + SIDE) % (2 * SIDE)

    firsts = [chunk_at(k, True) for k in range(n_first)]
    rests = [chunk_at(k, False) for k in range(n_rest)]

    def round_x(near, way):
        return (
            [(me, c) for c in rests]
            + [(me, c) for c in firsts]
            + [(near, c) for c in rests[way::2]]
            + [(across, c) for c in firsts]
            + [(near, c) for c in firsts[way::2]]
            + [(flip(near), c) for c in firsts[way::2]]
        )

    def from_x(near, way):
        return (
            [(near, c) for c in rests]
            + [(near, c) for c in firsts]
            + [(far, c) for c in rests[way::2]]
            + [(flip(near), c) for c in firsts]
            + [(far, c) for c in firsts[way::2]]
            + [(flip(far), c) for c in firsts[way::2]]
        )

    def over_z(own, one, two, three):
        return [(own, c) for c in firsts] + [(own, c) for c in rests] + [(r, c) for r in (one, two, three) for c in rests]

    goes = (round_x(left, 0), round_x(right, 1), over_z(me, left, right, far))
    comes = (from_x(left, 0), from_x(right, 1), over_z(across, flip(left), flip(right), flip(far)))
    targets = (right, left, across)
    slots = max(len(g) for g in goes)

    def line_wait():
        for hop in range(1, 2 * SIDE):
            source = (me + hop) % (2 * SIDE)
            pltpu.make_async_copy(line_place(source), line_place(source), line_got.at[source]).wait()

    def wide_wait():
        for hop in range(1, WIDE):
            source = land.at[:, (y + hop) % WIDE, core]
            pltpu.make_async_copy(source, source, wide_got.at[(y + hop) % WIDE]).wait()

    def router_step(step):
        if step == 0:
            line_wait()
        if step <= steps[0]:
            ring_step(step)
        if step == steps[0]:
            for hop in range(1, WIDE):
                wide_copy(hop).start()
        if step == steps[0] + 1:
            wide_wait()
            core_copy().start()
        if step == steps[0] + 2:
            theirs = land.at[:, :, 1 - core]
            pltpu.make_async_copy(theirs, theirs, core_got.at[0]).wait()
            for first in range(0, TALL * WIDE * CORES, 16):

                def line_in(k, _):
                    o = first + k
                    block[pl.ds(k, 1), :] = land[o // (WIDE * CORES), o // CORES % WIDE, o % CORES]
                    return 0

                lax.fori_loop(0, 16, line_in, 0)
                router[pl.ds(first, 16), :] = block[...].astype(jnp.bfloat16)

    def settle_pair(k):
        for chunks in (firsts, rests):
            if k < len(chunks):
                settle(*chunks[k])

    settle_pair(0)
    for slot in range(slots + BEHIND):
        settle_pair(slot + 1)
        if slot >= BEHIND:
            for came in comes:
                if slot - BEHIND < len(came):
                    source, (a, i) = came[slot - BEHIND]
                    arrived(source, a, i)
        for link in range(3):
            if slot < len(goes[link]):
                source, (a, i) = goes[link][slot]
                send(source, a, i, targets[link], link)
        if slot % APART == APART // 2 and slot // APART <= steps[0] + 2:
            router_step(slot // APART)

    for hop in range(1, 2 * SIDE):
        stat_copy(hop).wait_send()
        line_copy(hop).wait_send()
    for way in range(2):
        for step in range(steps[way]):
            ring_copy(way, step).wait_send()
    for hop in range(1, WIDE):
        wide_copy(hop).wait_send()
    core_copy().wait_send()
    for link in range(3):
        count = len(goes[link])
        all_sent = out.at[0, pl.ds(0, count * STEP), :]
        pltpu.make_async_copy(all_sent, all_sent, sent.at[link]).wait()


def place_kernel(gathered, scale, router, serve_gate, serve_up, scale_gate, scale_up, serve_router, done):
    copies = (
        pltpu.make_async_copy(gathered.at[pl.ds(0, 1)], serve_gate, done.at[0]),
        pltpu.make_async_copy(gathered.at[pl.ds(1, 1)], serve_up, done.at[1]),
        pltpu.make_async_copy(scale.at[pl.ds(0, 1)], scale_gate, done.at[2]),
        pltpu.make_async_copy(scale.at[pl.ds(1, 1)], scale_up, done.at[3]),
        pltpu.make_async_copy(router, serve_router, done.at[4]),
    )
    for copy in copies:
        copy.start()
    for copy in copies:
        copy.wait()


def shards(w_gate, avg_gate, w_up, avg_up, mix_share, router_weight, router_gain):
    _, share, width = w_gate.shape
    n = lax.axis_size("rows")
    in_hbm = pl.BlockSpec(memory_space=pltpu.HBM)
    in_vmem = pl.BlockSpec(memory_space=pltpu.VMEM)
    held = (w_gate, avg_gate, w_up, avg_up, router_weight.T, router_gain[None])
    owners = TALL * WIDE * CORES
    gathered, scale, router = pl.pallas_call(
        gather_kernel,
        out_shape=(
            jax.ShapeDtypeStruct((2, n * share, width), jnp.bfloat16),
            jax.ShapeDtypeStruct((2, width), jnp.float32),
            jax.ShapeDtypeStruct((owners, n * share), jnp.bfloat16),
        ),
        in_specs=[pl.BlockSpec(memory_space=pltpu.SMEM)] + [in_hbm] * 6,
        out_specs=(in_vmem,) * 3,
        scratch_shapes=[
            pltpu.VMEM((2, share, width), jnp.float32),
            pltpu.VMEM((2, share, width), jnp.float32),
            pltpu.VMEM((n, 2, width), jnp.float32),
            pltpu.VMEM((2, 1, share), jnp.float32),
            pltpu.VMEM((TALL, WIDE, CORES, 1, n * share), jnp.float32),
            pltpu.VMEM((16, n * share), jnp.float32),
            pltpu.SemaphoreType.DMA((6,)),
            pltpu.SemaphoreType.DMA((3,)),
            pltpu.SemaphoreType.DMA((n,)),
            pltpu.SemaphoreType.DMA((n,)),
            pltpu.SemaphoreType.DMA((n, 32)),
            pltpu.SemaphoreType.DMA((n,)),
            pltpu.SemaphoreType.DMA((n,)),
            pltpu.SemaphoreType.DMA((2, TALL // 2)),
            pltpu.SemaphoreType.DMA((2, TALL // 2)),
            pltpu.SemaphoreType.DMA((WIDE,)),
            pltpu.SemaphoreType.DMA((WIDE,)),
            pltpu.SemaphoreType.DMA((1,)),
            pltpu.SemaphoreType.DMA((1,)),
        ],
        compiler_params=pltpu.CompilerParams(collective_id=0, has_side_effects=True, vmem_limit_bytes=32 * 2**20),
        name="gather",
    )(mix_share, *(pltpu.with_memory_space_constraint(w, pltpu.HBM) for w in held))
    serve_gate, serve_up, scale_gate, scale_up, serve_router = pl.pallas_call(
        place_kernel,
        out_shape=(
            jax.ShapeDtypeStruct((1, n * share, width), jnp.bfloat16),
            jax.ShapeDtypeStruct((1, n * share, width), jnp.bfloat16),
            jax.ShapeDtypeStruct((1, width), jnp.float32),
            jax.ShapeDtypeStruct((1, width), jnp.float32),
            jax.ShapeDtypeStruct((owners, n * share), jnp.bfloat16),
        ),
        in_specs=[in_vmem] * 3,
        out_specs=(in_hbm,) * 5,
        scratch_shapes=[pltpu.SemaphoreType.DMA((5,))],
        compiler_params=pltpu.CompilerParams(vmem_limit_bytes=32 * 2**20),
        name="place",
    )(gathered, scale, router)
    return (serve_gate, serve_up, scale_gate, scale_up, serve_router.T)


def solution(mesh):
    placed = (
        P("owner", "rows", None),
        P("owner", "rows", None),
        P("owner", "rows", None),
        P("owner", "rows", None),
        P("owner"),
        P("rows", "owner"),
        P("rows"),
    )
    return jax.shard_map(
        shards,
        mesh=mesh,
        in_specs=placed,
        out_specs=(
            P("owner", None, None),
            P("owner", None, None),
            P("owner", None),
            P("owner", None),
            P(),
        ),
        check_vma=False,
    )
```

```python
import functools

import jax
import jax.numpy as jnp
from jax import lax
from jax.experimental import pallas as pl
from jax.experimental.pallas import tpu as pltpu
from jax.sharding import PartitionSpec as P

SIDE = 4
STEP = 16
TALL, WIDE, CORES = 8, 4, 2
BEHIND = 6
APART = 7
ACROSS = 9


def chunk_at(k, first):
    held = ACROSS if first else 16 - ACROSS
    return k // held, k % held + (0 if first else ACROSS)


def gather_kernel(
    mix, w_gate, avg_gate, w_up, avg_up, weight, gain,
    out, scale, router,
    fresh, other, stats, line, land, block,
    load, sent, stat_sent, stat_got, got,
    line_sent, line_got, z_sent, z_got, wide_sent, wide_got, core_sent, core_got,
):
    me = lax.axis_index("rows")
    owner = lax.axis_index("owner")
    high, y, core = owner // (WIDE * CORES), owner // CORES % WIDE, owner % CORES
    x, z = me % SIDE, me // SIDE
    right, left = z * SIDE + (x + 1) % SIDE, z * SIDE + (x + SIDE - 1) % SIDE
    across = (1 - z) * SIDE + x
    far = z * SIDE + (x + 2) % SIDE
    share = fresh.shape[1]
    n_first, n_rest = 2 * ACROSS, 2 * (16 - ACROSS)

    def at_owner(h, j, c):
        return {"owner": (h * WIDE + j) * CORES + c}

    loads = []
    for i, (source, target) in enumerate(
        (
            (w_gate.at[0], fresh.at[0]),
            (avg_gate.at[0], other.at[0]),
            (w_up.at[0], fresh.at[1]),
            (avg_up.at[0], other.at[1]),
            (weight, line.at[0]),
            (gain, line.at[1]),
        )
    ):
        loads.append(pltpu.make_async_copy(source, target, load.at[i]))
        loads[-1].start()

    barrier = pltpu.get_barrier_semaphore()
    for hop in range(1, 2 * SIDE):
        pl.semaphore_signal(barrier, inc=1, device_id={"rows": (me + hop) % (2 * SIDE)}, device_id_type=pl.DeviceIdType.MESH)

    above, below = high < TALL - 1, high > 0
    for there, step in ((above, 1), (below, -1)):

        @pl.when(there)
        def _():
            target = at_owner(high + step, y, core)
            pl.semaphore_signal(barrier, inc=1, device_id=target, device_id_type=pl.DeviceIdType.MESH)

    others = [at_owner(high, (y + hop) % WIDE, core) for hop in range(1, WIDE)]
    others.append(at_owner(high, y, 1 - core))
    for target in others:
        pl.semaphore_signal(barrier, inc=1, device_id=target, device_id_type=pl.DeviceIdType.MESH)

    part = mix[0]
    for a in range(2):
        loads[2 * a].wait()
        loads[2 * a + 1].wait()

        def mixed(i, total):
            rows = pl.ds(pl.multiple_of(i * 8, 8), 8)
            value = part * fresh[a, rows, :] + (1.0 - part) * other[a, rows, :]
            fresh[a, rows, :] = value
            return total + value * value

        total = lax.fori_loop(0, share // 8, mixed, jnp.zeros((8, fresh.shape[2]), jnp.float32), unroll=4)
        stats[me, pl.ds(a, 1), :] = jnp.sum(total, axis=0, keepdims=True)

    loads[4].wait()
    loads[5].wait()
    lanes = pl.ds(pl.multiple_of(me * share, share), share)
    land[high, y, core, :, lanes] = (line[0] * line[1]).astype(jnp.bfloat16).astype(jnp.float32)

    greeted = 2 * SIDE - 1 + len(others) + above.astype(jnp.int32) + below.astype(jnp.int32)
    pl.semaphore_wait(barrier, greeted)

    def stat_copy(hop):
        return pltpu.make_async_remote_copy(
            src_ref=stats.at[me],
            dst_ref=stats.at[me],
            send_sem=stat_sent.at[hop],
            recv_sem=stat_got.at[me],
            device_id={"rows": (me + hop) % (2 * SIDE)},
            device_id_type=pl.DeviceIdType.MESH,
        )

    def remote(place, send_sem, recv_sem, target):
        return pltpu.make_async_remote_copy(
            src_ref=place,
            dst_ref=place,
            send_sem=send_sem,
            recv_sem=recv_sem,
            device_id=target,
            device_id_type=pl.DeviceIdType.MESH,
        )

    def line_place(source):
        return land.at[high, y, core, :, pl.ds(pl.multiple_of(source * share, share), share)]

    def line_copy(hop):
        return remote(line_place(me), line_sent.at[hop], line_got.at[me], {"rows": (me + hop) % (2 * SIDE)})

    def z_copy(way, step):
        towards = 1 - 2 * way
        target = at_owner(high + towards, y, core)
        return remote(land.at[high - towards * step, y, core], z_sent.at[way, step], z_got.at[way, step], target)

    def z_sends(way, step):
        return (above & (high >= step)) if way == 0 else (below & (high + step <= TALL - 1))

    def z_comes(way, step):
        return (high >= step + 1) if way == 0 else (high + step + 1 <= TALL - 1)

    def z_step(step):
        for way in range(2):
            if step > 0:

                @pl.when(z_comes(way, step - 1))
                def _():
                    tile = land.at[high - (1 - 2 * way) * step, y, core]
                    pltpu.make_async_copy(tile, tile, z_got.at[way, step - 1]).wait()

            if step < TALL - 1:

                @pl.when(z_sends(way, step))
                def _():
                    z_copy(way, step).start()

    def wide_copy(hop):
        target = at_owner(high, (y + hop) % WIDE, core)
        return remote(land.at[:, y, core], wide_sent.at[hop], wide_got.at[y], target)

    def core_copy():
        return remote(land.at[:, :, core], core_sent.at[0], core_got.at[0], at_owner(high, y, 1 - core))

    for hop in range(1, 2 * SIDE):
        stat_copy(hop).start()
    for hop in range(1, 2 * SIDE):
        line_copy(hop).start()
    for hop in range(1, 2 * SIDE):
        source = (me + hop) % (2 * SIDE)
        pltpu.make_async_copy(stats.at[source], stats.at[source], stat_got.at[source]).wait()
    total = stats[0]
    for source in range(1, 2 * SIDE):
        total = total + stats[source]
    scale[...] = jnp.sqrt(total)

    def place(source, a, i):
        return out.at[a, pl.ds(pl.multiple_of(source * share + i * STEP, STEP), STEP), :]

    def send(source, a, i, target, link):
        pltpu.make_async_remote_copy(
            src_ref=place(source, a, i),
            dst_ref=place(source, a, i),
            send_sem=sent.at[link],
            recv_sem=got.at[source, a * 16 + i],
            device_id={"rows": target},
            device_id_type=pl.DeviceIdType.MESH,
        ).start()

    def arrived(source, a, i):
        pltpu.make_async_copy(place(source, a, i), place(source, a, i), got.at[source, a * 16 + i]).wait()

    def settle(a, i):
        rows = pl.ds(pl.multiple_of(i * STEP, STEP), STEP)
        value = fresh[a, rows, :] / scale[pl.ds(a, 1), :]
        out[a, pl.ds(pl.multiple_of(me * share + i * STEP, STEP), STEP), :] = value.astype(jnp.bfloat16)

    def flip(r):
        return (r + SIDE) % (2 * SIDE)

    firsts = [chunk_at(k, True) for k in range(n_first)]
    rests = [chunk_at(k, False) for k in range(n_rest)]

    def round_x(near, way):
        return (
            [(me, c) for c in rests]
            + [(me, c) for c in firsts]
            + [(near, c) for c in rests[way::2]]
            + [(across, c) for c in firsts]
            + [(near, c) for c in firsts[way::2]]
            + [(flip(near), c) for c in firsts[way::2]]
        )

    def from_x(near, way):
        return (
            [(near, c) for c in rests]
            + [(near, c) for c in firsts]
            + [(far, c) for c in rests[way::2]]
            + [(flip(near), c) for c in firsts]
            + [(far, c) for c in firsts[way::2]]
            + [(flip(far), c) for c in firsts[way::2]]
        )

    def over_z(own, one, two, three):
        return [(own, c) for c in firsts] + [(own, c) for c in rests] + [(r, c) for r in (one, two, three) for c in rests]

    goes = (round_x(left, 0), round_x(right, 1), over_z(me, left, right, far))
    comes = (from_x(left, 0), from_x(right, 1), over_z(across, flip(left), flip(right), flip(far)))
    targets = (right, left, across)
    slots = max(len(g) for g in goes)

    def line_wait():
        for hop in range(1, 2 * SIDE):
            source = (me + hop) % (2 * SIDE)
            pltpu.make_async_copy(line_place(source), line_place(source), line_got.at[source]).wait()

    def wide_wait():
        for hop in range(1, WIDE):
            source = land.at[:, (y + hop) % WIDE, core]
            pltpu.make_async_copy(source, source, wide_got.at[(y + hop) % WIDE]).wait()

    def router_step(step):
        if step == 0:
            line_wait()
        if step < TALL:
            z_step(step)
        if step == TALL - 1:
            for hop in range(1, WIDE):
                wide_copy(hop).start()
        if step == TALL:
            wide_wait()
            core_copy().start()
        if step == TALL + 1:
            theirs = land.at[:, :, 1 - core]
            pltpu.make_async_copy(theirs, theirs, core_got.at[0]).wait()
            for first in range(0, TALL * WIDE * CORES, 16):

                def line_in(k, _):
                    o = first + k
                    block[pl.ds(k, 1), :] = land[o // (WIDE * CORES), o // CORES % WIDE, o % CORES]
                    return 0

                lax.fori_loop(0, 16, line_in, 0)
                router[pl.ds(first, 16), :] = block[...].astype(jnp.bfloat16)

    def settle_pair(k):
        for chunks in (firsts, rests):
            if k < len(chunks):
                settle(*chunks[k])

    settle_pair(0)
    for slot in range(slots + BEHIND):
        settle_pair(slot + 1)
        if slot >= BEHIND:
            for came in comes:
                if slot - BEHIND < len(came):
                    source, (a, i) = came[slot - BEHIND]
                    arrived(source, a, i)
        if slot % APART == APART // 2 and slot // APART <= TALL + 1:
            router_step(slot // APART)
        for link in range(3):
            if slot < len(goes[link]):
                source, (a, i) = goes[link][slot]
                send(source, a, i, targets[link], link)

    for hop in range(1, 2 * SIDE):
        stat_copy(hop).wait_send()
        line_copy(hop).wait_send()
    for way in range(2):
        for step in range(TALL - 1):

            @pl.when(z_sends(way, step))
            def _():
                z_copy(way, step).wait_send()

    for hop in range(1, WIDE):
        wide_copy(hop).wait_send()
    core_copy().wait_send()
    for link in range(3):
        count = len(goes[link])
        all_sent = out.at[0, pl.ds(0, count * STEP), :]
        pltpu.make_async_copy(all_sent, all_sent, sent.at[link]).wait()


def place_kernel(gathered, scale, router, serve_gate, serve_up, scale_gate, scale_up, serve_router, done):
    copies = (
        pltpu.make_async_copy(gathered.at[pl.ds(0, 1)], serve_gate, done.at[0]),
        pltpu.make_async_copy(gathered.at[pl.ds(1, 1)], serve_up, done.at[1]),
        pltpu.make_async_copy(scale.at[pl.ds(0, 1)], scale_gate, done.at[2]),
        pltpu.make_async_copy(scale.at[pl.ds(1, 1)], scale_up, done.at[3]),
        pltpu.make_async_copy(router, serve_router, done.at[4]),
    )
    for copy in copies:
        copy.start()
    for copy in copies:
        copy.wait()


def shards(w_gate, avg_gate, w_up, avg_up, mix_share, router_weight, router_gain):
    _, share, width = w_gate.shape
    n = lax.axis_size("rows")
    in_hbm = pl.BlockSpec(memory_space=pltpu.HBM)
    in_vmem = pl.BlockSpec(memory_space=pltpu.VMEM)
    held = (w_gate, avg_gate, w_up, avg_up, router_weight.T, router_gain[None])
    owners = TALL * WIDE * CORES
    gathered, scale, router = pl.pallas_call(
        gather_kernel,
        out_shape=(
            jax.ShapeDtypeStruct((2, n * share, width), jnp.bfloat16),
            jax.ShapeDtypeStruct((2, width), jnp.float32),
            jax.ShapeDtypeStruct((owners, n * share), jnp.bfloat16),
        ),
        in_specs=[pl.BlockSpec(memory_space=pltpu.SMEM)] + [in_hbm] * 6,
        out_specs=(in_vmem,) * 3,
        scratch_shapes=[
            pltpu.VMEM((2, share, width), jnp.float32),
            pltpu.VMEM((2, share, width), jnp.float32),
            pltpu.VMEM((n, 2, width), jnp.float32),
            pltpu.VMEM((2, 1, share), jnp.float32),
            pltpu.VMEM((TALL, WIDE, CORES, 1, n * share), jnp.float32),
            pltpu.VMEM((16, n * share), jnp.float32),
            pltpu.SemaphoreType.DMA((6,)),
            pltpu.SemaphoreType.DMA((3,)),
            pltpu.SemaphoreType.DMA((n,)),
            pltpu.SemaphoreType.DMA((n,)),
            pltpu.SemaphoreType.DMA((n, 32)),
            pltpu.SemaphoreType.DMA((n,)),
            pltpu.SemaphoreType.DMA((n,)),
            pltpu.SemaphoreType.DMA((2, TALL - 1)),
            pltpu.SemaphoreType.DMA((2, TALL - 1)),
            pltpu.SemaphoreType.DMA((WIDE,)),
            pltpu.SemaphoreType.DMA((WIDE,)),
            pltpu.SemaphoreType.DMA((1,)),
            pltpu.SemaphoreType.DMA((1,)),
        ],
        compiler_params=pltpu.CompilerParams(collective_id=0, has_side_effects=True, vmem_limit_bytes=32 * 2**20),
        name="gather",
    )(mix_share, *(pltpu.with_memory_space_constraint(w, pltpu.HBM) for w in held))
    serve_gate, serve_up, scale_gate, scale_up, serve_router = pl.pallas_call(
        place_kernel,
        out_shape=(
            jax.ShapeDtypeStruct((1, n * share, width), jnp.bfloat16),
            jax.ShapeDtypeStruct((1, n * share, width), jnp.bfloat16),
            jax.ShapeDtypeStruct((1, width), jnp.float32),
            jax.ShapeDtypeStruct((1, width), jnp.float32),
            jax.ShapeDtypeStruct((owners, n * share), jnp.bfloat16),
        ),
        in_specs=[in_vmem] * 3,
        out_specs=(in_hbm,) * 5,
        scratch_shapes=[pltpu.SemaphoreType.DMA((5,))],
        compiler_params=pltpu.CompilerParams(vmem_limit_bytes=32 * 2**20),
        name="place",
    )(gathered, scale, router)
    return (serve_gate, serve_up, scale_gate, scale_up, serve_router.T)


def solution(mesh):
    placed = (
        P("owner", "rows", None),
        P("owner", "rows", None),
        P("owner", "rows", None),
        P("owner", "rows", None),
        P("owner"),
        P("rows", "owner"),
        P("rows"),
    )
    return jax.shard_map(
        shards,
        mesh=mesh,
        in_specs=placed,
        out_specs=(
            P("owner", None, None),
            P("owner", None, None),
            P("owner", None),
            P("owner", None),
            P(),
        ),
        check_vma=False,
    )
```

```python
import functools

import jax
import jax.numpy as jnp
from jax import lax
from jax.experimental import pallas as pl
from jax.experimental.pallas import tpu as pltpu
from jax.sharding import PartitionSpec as P

SIDE = 4
STEP = 16
TALL, WIDE, CORES = 8, 4, 2
BEHIND = 6
APART = 7
ACROSS = 9


def chunk_at(k, first):
    held = ACROSS if first else 16 - ACROSS
    return k // held, k % held + (0 if first else ACROSS)


def gather_kernel(
    mix, w_gate, avg_gate, w_up, avg_up, weight, gain,
    out, scale, router,
    fresh, other, stats, line, land, block,
    load, sent, stat_sent, stat_got, got,
    line_sent, line_got, z_sent, z_got, wide_sent, wide_got, core_sent, core_got,
):
    me = lax.axis_index("rows")
    owner = lax.axis_index("owner")
    high, y, core = owner // (WIDE * CORES), owner // CORES % WIDE, owner % CORES
    x, z = me % SIDE, me // SIDE
    right, left = z * SIDE + (x + 1) % SIDE, z * SIDE + (x + SIDE - 1) % SIDE
    across = (1 - z) * SIDE + x
    far = z * SIDE + (x + 2) % SIDE
    share = fresh.shape[1]
    n_first, n_rest = 2 * ACROSS, 2 * (16 - ACROSS)

    def at_owner(h, j, c):
        return {"owner": (h * WIDE + j) * CORES + c}

    loads = []
    for i, (source, target) in enumerate(
        (
            (w_gate.at[0], fresh.at[0]),
            (avg_gate.at[0], other.at[0]),
            (w_up.at[0], fresh.at[1]),
            (avg_up.at[0], other.at[1]),
            (weight, line.at[0]),
            (gain, line.at[1]),
        )
    ):
        loads.append(pltpu.make_async_copy(source, target, load.at[i]))
        loads[-1].start()

    barrier = pltpu.get_barrier_semaphore()
    for hop in range(1, 2 * SIDE):
        pl.semaphore_signal(barrier, inc=1, device_id={"rows": (me + hop) % (2 * SIDE)}, device_id_type=pl.DeviceIdType.MESH)

    onward = 2 * z - 1
    for there, step, row in ((high < TALL - 1, 1, x), (high > 0, -1, SIDE + x)):

        @pl.when(there)
        def _():
            target = at_owner(high + step, y, core) | {"rows": row}
            pl.semaphore_signal(barrier, inc=1, device_id=target, device_id_type=pl.DeviceIdType.MESH)

    others = [at_owner(high, (y + hop) % WIDE, core) for hop in range(1, WIDE)]
    others.append(at_owner(high, y, 1 - core))
    for target in others:
        pl.semaphore_signal(barrier, inc=1, device_id=target, device_id_type=pl.DeviceIdType.MESH)

    part = mix[0]
    for a in range(2):
        loads[2 * a].wait()
        loads[2 * a + 1].wait()

        def mixed(i, total):
            rows = pl.ds(pl.multiple_of(i * 8, 8), 8)
            value = part * fresh[a, rows, :] + (1.0 - part) * other[a, rows, :]
            fresh[a, rows, :] = value
            return total + value * value

        total = lax.fori_loop(0, share // 8, mixed, jnp.zeros((8, fresh.shape[2]), jnp.float32), unroll=4)
        stats[me, pl.ds(a, 1), :] = jnp.sum(total, axis=0, keepdims=True)

    loads[4].wait()
    loads[5].wait()
    lanes = pl.ds(pl.multiple_of(me * share, share), share)
    land[high, y, core, :, lanes] = (line[0] * line[1]).astype(jnp.bfloat16).astype(jnp.float32)

    has_next = (high + onward >= 0) & (high + onward < TALL)
    greeted = 2 * SIDE - 1 + len(others) + 2 * has_next.astype(jnp.int32)
    pl.semaphore_wait(barrier, greeted)

    def stat_copy(hop):
        return pltpu.make_async_remote_copy(
            src_ref=stats.at[me],
            dst_ref=stats.at[me],
            send_sem=stat_sent.at[hop],
            recv_sem=stat_got.at[me],
            device_id={"rows": (me + hop) % (2 * SIDE)},
            device_id_type=pl.DeviceIdType.MESH,
        )

    def remote(place, send_sem, recv_sem, target):
        return pltpu.make_async_remote_copy(
            src_ref=place,
            dst_ref=place,
            send_sem=send_sem,
            recv_sem=recv_sem,
            device_id=target,
            device_id_type=pl.DeviceIdType.MESH,
        )

    def line_place(source):
        return land.at[high, y, core, :, pl.ds(pl.multiple_of(source * share, share), share)]

    def line_copy(hop):
        return remote(line_place(me), line_sent.at[hop], line_got.at[me], {"rows": (me + hop) % (2 * SIDE)})

    def z_copy(row, step):
        target = at_owner(high + onward, y, core) | {"rows": (me, across)[row]}
        return remote(land.at[high - onward * step, y, core], z_sent.at[row, step], z_got.at[1 - z, step], target)

    def z_sends(step):
        behind = high - onward * step
        return has_next & (behind >= 0) & (behind < TALL)

    def z_comes(way, step):
        return (high >= step + 1) if way == 0 else (high + step + 1 <= TALL - 1)

    def z_step(step):
        if step > 0:
            for way in range(2):

                @pl.when(z_comes(way, step - 1))
                def _():
                    tile = land.at[high - (1 - 2 * way) * step, y, core]
                    pltpu.make_async_copy(tile, tile, z_got.at[way, step - 1]).wait()

        if step < TALL - 1:

            @pl.when(z_sends(step))
            def _():
                for row in range(2):
                    z_copy(row, step).start()

    def wide_copy(hop):
        target = at_owner(high, (y + hop) % WIDE, core)
        return remote(land.at[:, y, core], wide_sent.at[hop], wide_got.at[y], target)

    def core_copy():
        return remote(land.at[:, :, core], core_sent.at[0], core_got.at[0], at_owner(high, y, 1 - core))

    for hop in range(1, 2 * SIDE):
        stat_copy(hop).start()
    for hop in range(1, 2 * SIDE):
        line_copy(hop).start()
    for hop in range(1, 2 * SIDE):
        source = (me + hop) % (2 * SIDE)
        pltpu.make_async_copy(stats.at[source], stats.at[source], stat_got.at[source]).wait()
    total = stats[0]
    for source in range(1, 2 * SIDE):
        total = total + stats[source]
    scale[...] = jnp.sqrt(total)

    def place(source, a, i):
        return out.at[a, pl.ds(pl.multiple_of(source * share + i * STEP, STEP), STEP), :]

    def send(source, a, i, target, link):
        pltpu.make_async_remote_copy(
            src_ref=place(source, a, i),
            dst_ref=place(source, a, i),
            send_sem=sent.at[link],
            recv_sem=got.at[source, a * 16 + i],
            device_id={"rows": target},
            device_id_type=pl.DeviceIdType.MESH,
        ).start()

    def arrived(source, a, i):
        pltpu.make_async_copy(place(source, a, i), place(source, a, i), got.at[source, a * 16 + i]).wait()

    def settle(a, i):
        rows = pl.ds(pl.multiple_of(i * STEP, STEP), STEP)
        value = fresh[a, rows, :] / scale[pl.ds(a, 1), :]
        out[a, pl.ds(pl.multiple_of(me * share + i * STEP, STEP), STEP), :] = value.astype(jnp.bfloat16)

    def flip(r):
        return (r + SIDE) % (2 * SIDE)

    firsts = [chunk_at(k, True) for k in range(n_first)]
    rests = [chunk_at(k, False) for k in range(n_rest)]

    def round_x(near, way):
        return (
            [(me, c) for c in rests]
            + [(me, c) for c in firsts]
            + [(near, c) for c in rests[way::2]]
            + [(across, c) for c in firsts]
            + [(near, c) for c in firsts[way::2]]
            + [(flip(near), c) for c in firsts[way::2]]
        )

    def from_x(near, way):
        return (
            [(near, c) for c in rests]
            + [(near, c) for c in firsts]
            + [(far, c) for c in rests[way::2]]
            + [(flip(near), c) for c in firsts]
            + [(far, c) for c in firsts[way::2]]
            + [(flip(far), c) for c in firsts[way::2]]
        )

    def over_z(own, one, two, three):
        return [(own, c) for c in firsts] + [(own, c) for c in rests] + [(r, c) for r in (one, two, three) for c in rests]

    goes = (round_x(left, 0), round_x(right, 1), over_z(me, left, right, far))
    comes = (from_x(left, 0), from_x(right, 1), over_z(across, flip(left), flip(right), flip(far)))
    targets = (right, left, across)
    slots = max(len(g) for g in goes)

    def line_wait():
        for hop in range(1, 2 * SIDE):
            source = (me + hop) % (2 * SIDE)
            pltpu.make_async_copy(line_place(source), line_place(source), line_got.at[source]).wait()

    def wide_wait():
        for hop in range(1, WIDE):
            source = land.at[:, (y + hop) % WIDE, core]
            pltpu.make_async_copy(source, source, wide_got.at[(y + hop) % WIDE]).wait()

    def router_step(step):
        if step == 0:
            line_wait()
        if step < TALL:
            z_step(step)
        if step == TALL - 1:
            for hop in range(1, WIDE):
                wide_copy(hop).start()
        if step == TALL:
            wide_wait()
            core_copy().start()
        if step == TALL + 1:
            theirs = land.at[:, :, 1 - core]
            pltpu.make_async_copy(theirs, theirs, core_got.at[0]).wait()
            for first in range(0, TALL * WIDE * CORES, 16):

                def line_in(k, _):
                    o = first + k
                    block[pl.ds(k, 1), :] = land[o // (WIDE * CORES), o // CORES % WIDE, o % CORES]
                    return 0

                lax.fori_loop(0, 16, line_in, 0)
                router[pl.ds(first, 16), :] = block[...].astype(jnp.bfloat16)

    def settle_pair(k):
        for chunks in (firsts, rests):
            if k < len(chunks):
                settle(*chunks[k])

    settle_pair(0)
    for slot in range(slots + BEHIND):
        settle_pair(slot + 1)
        if slot >= BEHIND:
            for came in comes:
                if slot - BEHIND < len(came):
                    source, (a, i) = came[slot - BEHIND]
                    arrived(source, a, i)
        if slot % APART == APART // 2 and slot // APART <= TALL + 1:
            router_step(slot // APART)
        for link in range(3):
            if slot < len(goes[link]):
                source, (a, i) = goes[link][slot]
                send(source, a, i, targets[link], link)

    for hop in range(1, 2 * SIDE):
        stat_copy(hop).wait_send()
        line_copy(hop).wait_send()
    for step in range(TALL - 1):

        @pl.when(z_sends(step))
        def _():
            for row in range(2):
                z_copy(row, step).wait_send()

    for hop in range(1, WIDE):
        wide_copy(hop).wait_send()
    core_copy().wait_send()
    for link in range(3):
        count = len(goes[link])
        all_sent = out.at[0, pl.ds(0, count * STEP), :]
        pltpu.make_async_copy(all_sent, all_sent, sent.at[link]).wait()


def place_kernel(gathered, scale, router, serve_gate, serve_up, scale_gate, scale_up, serve_router, done):
    copies = (
        pltpu.make_async_copy(gathered.at[pl.ds(0, 1)], serve_gate, done.at[0]),
        pltpu.make_async_copy(gathered.at[pl.ds(1, 1)], serve_up, done.at[1]),
        pltpu.make_async_copy(scale.at[pl.ds(0, 1)], scale_gate, done.at[2]),
        pltpu.make_async_copy(scale.at[pl.ds(1, 1)], scale_up, done.at[3]),
        pltpu.make_async_copy(router, serve_router, done.at[4]),
    )
    for copy in copies:
        copy.start()
    for copy in copies:
        copy.wait()


def shards(w_gate, avg_gate, w_up, avg_up, mix_share, router_weight, router_gain):
    _, share, width = w_gate.shape
    n = lax.axis_size("rows")
    in_hbm = pl.BlockSpec(memory_space=pltpu.HBM)
    in_vmem = pl.BlockSpec(memory_space=pltpu.VMEM)
    held = (w_gate, avg_gate, w_up, avg_up, router_weight.T, router_gain[None])
    owners = TALL * WIDE * CORES
    gathered, scale, router = pl.pallas_call(
        gather_kernel,
        out_shape=(
            jax.ShapeDtypeStruct((2, n * share, width), jnp.bfloat16),
            jax.ShapeDtypeStruct((2, width), jnp.float32),
            jax.ShapeDtypeStruct((owners, n * share), jnp.bfloat16),
        ),
        in_specs=[pl.BlockSpec(memory_space=pltpu.SMEM)] + [in_hbm] * 6,
        out_specs=(in_vmem,) * 3,
        scratch_shapes=[
            pltpu.VMEM((2, share, width), jnp.float32),
            pltpu.VMEM((2, share, width), jnp.float32),
            pltpu.VMEM((n, 2, width), jnp.float32),
            pltpu.VMEM((2, 1, share), jnp.float32),
            pltpu.VMEM((TALL, WIDE, CORES, 1, n * share), jnp.float32),
            pltpu.VMEM((16, n * share), jnp.float32),
            pltpu.SemaphoreType.DMA((6,)),
            pltpu.SemaphoreType.DMA((3,)),
            pltpu.SemaphoreType.DMA((n,)),
            pltpu.SemaphoreType.DMA((n,)),
            pltpu.SemaphoreType.DMA((n, 32)),
            pltpu.SemaphoreType.DMA((n,)),
            pltpu.SemaphoreType.DMA((n,)),
            pltpu.SemaphoreType.DMA((2, TALL - 1)),
            pltpu.SemaphoreType.DMA((2, TALL - 1)),
            pltpu.SemaphoreType.DMA((WIDE,)),
            pltpu.SemaphoreType.DMA((WIDE,)),
            pltpu.SemaphoreType.DMA((1,)),
            pltpu.SemaphoreType.DMA((1,)),
        ],
        compiler_params=pltpu.CompilerParams(collective_id=0, has_side_effects=True, vmem_limit_bytes=32 * 2**20),
        name="gather",
    )(mix_share, *(pltpu.with_memory_space_constraint(w, pltpu.HBM) for w in held))
    serve_gate, serve_up, scale_gate, scale_up, serve_router = pl.pallas_call(
        place_kernel,
        out_shape=(
            jax.ShapeDtypeStruct((1, n * share, width), jnp.bfloat16),
            jax.ShapeDtypeStruct((1, n * share, width), jnp.bfloat16),
            jax.ShapeDtypeStruct((1, width), jnp.float32),
            jax.ShapeDtypeStruct((1, width), jnp.float32),
            jax.ShapeDtypeStruct((owners, n * share), jnp.bfloat16),
        ),
        in_specs=[in_vmem] * 3,
        out_specs=(in_hbm,) * 5,
        scratch_shapes=[pltpu.SemaphoreType.DMA((5,))],
        compiler_params=pltpu.CompilerParams(vmem_limit_bytes=32 * 2**20),
        name="place",
    )(gathered, scale, router)
    return (serve_gate, serve_up, scale_gate, scale_up, serve_router.T)


def solution(mesh):
    placed = (
        P("owner", "rows", None),
        P("owner", "rows", None),
        P("owner", "rows", None),
        P("owner", "rows", None),
        P("owner"),
        P("rows", "owner"),
        P("rows"),
    )
    return jax.shard_map(
        shards,
        mesh=mesh,
        in_specs=placed,
        out_specs=(
            P("owner", None, None),
            P("owner", None, None),
            P("owner", None),
            P("owner", None),
            P(),
        ),
        check_vma=False,
    )
```

```python
import functools

import jax
import jax.numpy as jnp
from jax import lax
from jax.experimental import pallas as pl
from jax.experimental.pallas import tpu as pltpu
from jax.sharding import PartitionSpec as P

SIDE = 4
STEP = 16
TALL, WIDE, CORES = 8, 4, 2
BEHIND = 16
APART = 7
SPREAD = 172.0
ACROSS = 9


def chunk_at(k, first):
    held = ACROSS if first else 16 - ACROSS
    return k // held, k % held + (0 if first else ACROSS)


def gather_kernel(
    mix, w_gate, avg_gate, w_up, avg_up, weight, gain,
    out, scale, router,
    coded, fresh, other, stats, factor, line, land, block,
    load, sent, stat_sent, stat_got, got,
    line_sent, line_got, z_sent, z_got, wide_sent, wide_got, core_sent, core_got,
):
    me = lax.axis_index("rows")
    owner = lax.axis_index("owner")
    high, y, core = owner // (WIDE * CORES), owner // CORES % WIDE, owner % CORES
    x, z = me % SIDE, me // SIDE
    right, left = z * SIDE + (x + 1) % SIDE, z * SIDE + (x + SIDE - 1) % SIDE
    across = (1 - z) * SIDE + x
    far = z * SIDE + (x + 2) % SIDE
    share = fresh.shape[1]
    n_first, n_rest = 2 * ACROSS, 2 * (16 - ACROSS)

    def at_owner(h, j, c):
        return {"owner": (h * WIDE + j) * CORES + c}

    loads = []
    for i, (source, target) in enumerate(
        (
            (w_gate.at[0], fresh.at[0]),
            (avg_gate.at[0], other.at[0]),
            (w_up.at[0], fresh.at[1]),
            (avg_up.at[0], other.at[1]),
            (weight, line.at[0]),
            (gain, line.at[1]),
        )
    ):
        loads.append(pltpu.make_async_copy(source, target, load.at[i]))
        loads[-1].start()

    barrier = pltpu.get_barrier_semaphore()
    for hop in range(1, 2 * SIDE):
        pl.semaphore_signal(barrier, inc=1, device_id={"rows": (me + hop) % (2 * SIDE)}, device_id_type=pl.DeviceIdType.MESH)

    onward = 2 * z - 1
    for there, step, row in ((high < TALL - 1, 1, x), (high > 0, -1, SIDE + x)):

        @pl.when(there)
        def _():
            target = at_owner(high + step, y, core) | {"rows": row}
            pl.semaphore_signal(barrier, inc=1, device_id=target, device_id_type=pl.DeviceIdType.MESH)

    others = [at_owner(high, (y + hop) % WIDE, core) for hop in range(1, WIDE)]
    others.append(at_owner(high, y, 1 - core))
    for target in others:
        pl.semaphore_signal(barrier, inc=1, device_id=target, device_id_type=pl.DeviceIdType.MESH)

    part = mix[0]
    for a in range(2):
        loads[2 * a].wait()
        loads[2 * a + 1].wait()

        def mixed(i, total):
            rows = pl.ds(pl.multiple_of(i * 8, 8), 8)
            value = part * fresh[a, rows, :] + (1.0 - part) * other[a, rows, :]
            fresh[a, rows, :] = value
            return total + value * value

        total = lax.fori_loop(0, share // 8, mixed, jnp.zeros((8, fresh.shape[2]), jnp.float32), unroll=4)
        stats[me, pl.ds(a, 1), :] = jnp.sum(total, axis=0, keepdims=True)

    loads[4].wait()
    loads[5].wait()
    lanes = pl.ds(pl.multiple_of(me * share, share), share)
    land[high, y, core, :, lanes] = (line[0] * line[1]).astype(jnp.bfloat16).astype(jnp.float32)

    has_next = (high + onward >= 0) & (high + onward < TALL)
    greeted = 2 * SIDE - 1 + len(others) + 2 * has_next.astype(jnp.int32)
    pl.semaphore_wait(barrier, greeted)

    def stat_copy(hop):
        return pltpu.make_async_remote_copy(
            src_ref=stats.at[me],
            dst_ref=stats.at[me],
            send_sem=stat_sent.at[hop],
            recv_sem=stat_got.at[me],
            device_id={"rows": (me + hop) % (2 * SIDE)},
            device_id_type=pl.DeviceIdType.MESH,
        )

    def remote(place, send_sem, recv_sem, target):
        return pltpu.make_async_remote_copy(
            src_ref=place,
            dst_ref=place,
            send_sem=send_sem,
            recv_sem=recv_sem,
            device_id=target,
            device_id_type=pl.DeviceIdType.MESH,
        )

    def line_place(source):
        return land.at[high, y, core, :, pl.ds(pl.multiple_of(source * share, share), share)]

    def line_copy(hop):
        return remote(line_place(me), line_sent.at[hop], line_got.at[me], {"rows": (me + hop) % (2 * SIDE)})

    def z_copy(row, step):
        target = at_owner(high + onward, y, core) | {"rows": (me, across)[row]}
        return remote(land.at[high - onward * step, y, core], z_sent.at[row, step], z_got.at[1 - z, step], target)

    def z_sends(step):
        behind = high - onward * step
        return has_next & (behind >= 0) & (behind < TALL)

    def z_comes(way, step):
        return (high >= step + 1) if way == 0 else (high + step + 1 <= TALL - 1)

    def z_step(step):
        if step > 0:
            for way in range(2):

                @pl.when(z_comes(way, step - 1))
                def _():
                    tile = land.at[high - (1 - 2 * way) * step, y, core]
                    pltpu.make_async_copy(tile, tile, z_got.at[way, step - 1]).wait()

        if step < TALL - 1:

            @pl.when(z_sends(step))
            def _():
                for row in range(2):
                    z_copy(row, step).start()

    def wide_copy(hop):
        target = at_owner(high, (y + hop) % WIDE, core)
        return remote(land.at[:, y, core], wide_sent.at[hop], wide_got.at[y], target)

    def core_copy():
        return remote(land.at[:, :, core], core_sent.at[0], core_got.at[0], at_owner(high, y, 1 - core))

    for hop in range(1, 2 * SIDE):
        stat_copy(hop).start()
    for hop in range(1, 2 * SIDE):
        line_copy(hop).start()
    def norms():
        for hop in range(1, 2 * SIDE):
            source = (me + hop) % (2 * SIDE)
            pltpu.make_async_copy(stats.at[source], stats.at[source], stat_got.at[source]).wait()
        total = stats[0]
        for source in range(1, 2 * SIDE):
            total = total + stats[source]
        scale[...] = jnp.sqrt(total)
        for source in range(2 * SIDE):
            factor[source] = jnp.sqrt(stats[source]) / scale[...]

    def place(source, a, i):
        return coded.at[a, pl.ds(pl.multiple_of(source * share + i * STEP, STEP), STEP), :]

    def send(source, a, i, target, link):
        pltpu.make_async_remote_copy(
            src_ref=place(source, a, i),
            dst_ref=place(source, a, i),
            send_sem=sent.at[link],
            recv_sem=got.at[source, a * 16 + i],
            device_id={"rows": target},
            device_id_type=pl.DeviceIdType.MESH,
        ).start()

    def arrived(source, a, i):
        pltpu.make_async_copy(place(source, a, i), place(source, a, i), got.at[source, a * 16 + i]).wait()

    def rows_of(source, i):
        return pl.ds(pl.multiple_of(source * share + i * STEP, STEP), STEP)

    def own_norm(a):
        total = stats[me, pl.ds(a, 1), :]
        return jnp.where(total > 0.0, 1.0 / jnp.sqrt(total), 0.0)

    over = (own_norm(0), own_norm(1))

    def encode(a, i):
        value = fresh[a, pl.ds(i * STEP, STEP), :]
        size = jnp.exp(SPREAD * jnp.sqrt(jnp.abs(value) * over[a]) - 0.5 * SPREAD)
        coded[a, rows_of(me, i), :] = jnp.where(value < 0.0, -size, size).astype(jnp.bfloat16)

    def decode(source, a, i):
        code = coded[a, rows_of(source, i), :].astype(jnp.float32)
        root = jnp.log(jnp.abs(code)) * (1.0 / SPREAD) + 0.5
        size = root * root * factor[source, pl.ds(a, 1), :]
        out[a, rows_of(source, i), :] = jnp.where(code < 0.0, -size, size).astype(jnp.bfloat16)

    def settle(k, _):
        a, i = k // 16, k % 16
        value = fresh[a, rows_of(0, i), :] / scale[pl.ds(a, 1), :]
        out[a, rows_of(me, i), :] = value.astype(jnp.bfloat16)
        return 0

    def flip(r):
        return (r + SIDE) % (2 * SIDE)

    firsts = [(True, k) for k in range(n_first)]
    rests = [(False, k) for k in range(n_rest)]

    def round_x(near, way):
        return (
            [(me, c) for c in rests]
            + [(me, c) for c in firsts]
            + [(near, c) for c in rests[way::2]]
            + [(across, c) for c in firsts]
            + [(near, c) for c in firsts[way::2]]
            + [(flip(near), c) for c in firsts[way::2]]
        )

    def from_x(near, way):
        return (
            (near, rests),
            (near, firsts),
            (far, rests[way::2]),
            (flip(near), firsts),
            (far, firsts[way::2]),
            (flip(far), firsts[way::2]),
        )

    def over_z(own, one, two, three):
        return ((own, firsts), (own, rests), (one, rests), (two, rests), (three, rests))

    goes = (
        round_x(left, 0),
        round_x(right, 1),
        [(source, c) for source, run in over_z(me, left, right, far) for c in run],
    )
    runs = (from_x(left, 0), from_x(right, 1), over_z(across, flip(left), flip(right), flip(far)))
    comes = tuple([(source, run, at) for source, run in each for at in range(len(run))] for each in runs)

    def decode_run(source, run, begin, end):
        first, k = run[begin]
        stride = run[1][1] - run[0][1]

        def one(j, _):
            decode(source, *chunk_at(k + stride * j, first))
            return 0

        lax.fori_loop(0, end - begin, one, 0)

    targets = (right, left, across)
    slots = max(len(g) for g in goes)

    def line_wait():
        for hop in range(1, 2 * SIDE):
            source = (me + hop) % (2 * SIDE)
            pltpu.make_async_copy(line_place(source), line_place(source), line_got.at[source]).wait()

    def wide_wait():
        for hop in range(1, WIDE):
            source = land.at[:, (y + hop) % WIDE, core]
            pltpu.make_async_copy(source, source, wide_got.at[(y + hop) % WIDE]).wait()

    def router_step(step):
        if step == 0:
            line_wait()
        if step < TALL:
            z_step(step)
        if step == TALL - 1:
            for hop in range(1, WIDE):
                wide_copy(hop).start()
        if step == TALL:
            wide_wait()
            core_copy().start()
        if step == TALL + 1:
            theirs = land.at[:, :, 1 - core]
            pltpu.make_async_copy(theirs, theirs, core_got.at[0]).wait()
            for first in range(0, TALL * WIDE * CORES, 16):

                def line_in(k, _):
                    o = first + k
                    block[pl.ds(k, 1), :] = land[o // (WIDE * CORES), o // CORES % WIDE, o % CORES]
                    return 0

                lax.fori_loop(0, 16, line_in, 0)
                router[pl.ds(first, 16), :] = block[...].astype(jnp.bfloat16)

    def encode_pair(k):
        for chunks in (firsts, rests):
            if k < len(chunks):
                first, at = chunks[k]
                encode(*chunk_at(at, first))

    encode_pair(0)
    waiting = [0, 0, 0]
    for slot in range(slots + BEHIND):
        encode_pair(slot + 1)
        if slot == BEHIND - 4:
            norms()
        if slot in range(BEHIND + 2, BEHIND + 18, 2):
            at = (slot - BEHIND - 2) * 2
            lax.fori_loop(at, at + 4, settle, 0)
        for link in range(3):
            at = slot - BEHIND
            if 0 <= at < len(comes[link]):
                source, run, j = comes[link][at]
                arrived(source, *chunk_at(run[j][1], run[j][0]))
                waiting[link] += 1
                if waiting[link] == 6 or j == len(run) - 1 or at >= slots - 4:
                    decode_run(source, run, j + 1 - waiting[link], j + 1)
                    waiting[link] = 0
        if slot % APART == APART // 2 and slot // APART <= TALL + 1:
            router_step(slot // APART)
        for link in range(3):
            if slot < len(goes[link]):
                source, (first, at) = goes[link][slot]
                send(source, *chunk_at(at, first), targets[link], link)

    for hop in range(1, 2 * SIDE):
        stat_copy(hop).wait_send()
        line_copy(hop).wait_send()
    for step in range(TALL - 1):

        @pl.when(z_sends(step))
        def _():
            for row in range(2):
                z_copy(row, step).wait_send()

    for hop in range(1, WIDE):
        wide_copy(hop).wait_send()
    core_copy().wait_send()
    for link in range(3):
        count = len(goes[link])
        all_sent = coded.at[0, pl.ds(0, count * STEP), :]
        pltpu.make_async_copy(all_sent, all_sent, sent.at[link]).wait()


def place_kernel(gathered, scale, router, serve_gate, serve_up, scale_gate, scale_up, serve_router, done):
    copies = (
        pltpu.make_async_copy(gathered.at[pl.ds(0, 1)], serve_gate, done.at[0]),
        pltpu.make_async_copy(gathered.at[pl.ds(1, 1)], serve_up, done.at[1]),
        pltpu.make_async_copy(scale.at[pl.ds(0, 1)], scale_gate, done.at[2]),
        pltpu.make_async_copy(scale.at[pl.ds(1, 1)], scale_up, done.at[3]),
        pltpu.make_async_copy(router, serve_router, done.at[4]),
    )
    for copy in copies:
        copy.start()
    for copy in copies:
        copy.wait()


def shards(w_gate, avg_gate, w_up, avg_up, mix_share, router_weight, router_gain):
    _, share, width = w_gate.shape
    n = lax.axis_size("rows")
    in_hbm = pl.BlockSpec(memory_space=pltpu.HBM)
    in_vmem = pl.BlockSpec(memory_space=pltpu.VMEM)
    held = (w_gate, avg_gate, w_up, avg_up, router_weight.T, router_gain[None])
    owners = TALL * WIDE * CORES
    gathered, scale, router = pl.pallas_call(
        gather_kernel,
        out_shape=(
            jax.ShapeDtypeStruct((2, n * share, width), jnp.bfloat16),
            jax.ShapeDtypeStruct((2, width), jnp.float32),
            jax.ShapeDtypeStruct((owners, n * share), jnp.bfloat16),
        ),
        in_specs=[pl.BlockSpec(memory_space=pltpu.SMEM)] + [in_hbm] * 6,
        out_specs=(in_vmem,) * 3,
        scratch_shapes=[
            pltpu.VMEM((2, n * share, width), jnp.bfloat16),
            pltpu.VMEM((2, share, width), jnp.float32),
            pltpu.VMEM((2, share, width), jnp.float32),
            pltpu.VMEM((n, 2, width), jnp.float32),
            pltpu.VMEM((n, 2, width), jnp.float32),
            pltpu.VMEM((2, 1, share), jnp.float32),
            pltpu.VMEM((TALL, WIDE, CORES, 1, n * share), jnp.float32),
            pltpu.VMEM((16, n * share), jnp.float32),
            pltpu.SemaphoreType.DMA((6,)),
            pltpu.SemaphoreType.DMA((3,)),
            pltpu.SemaphoreType.DMA((n,)),
            pltpu.SemaphoreType.DMA((n,)),
            pltpu.SemaphoreType.DMA((n, 32)),
            pltpu.SemaphoreType.DMA((n,)),
            pltpu.SemaphoreType.DMA((n,)),
            pltpu.SemaphoreType.DMA((2, TALL - 1)),
            pltpu.SemaphoreType.DMA((2, TALL - 1)),
            pltpu.SemaphoreType.DMA((WIDE,)),
            pltpu.SemaphoreType.DMA((WIDE,)),
            pltpu.SemaphoreType.DMA((1,)),
            pltpu.SemaphoreType.DMA((1,)),
        ],
        compiler_params=pltpu.CompilerParams(collective_id=0, has_side_effects=True, vmem_limit_bytes=32 * 2**20),
        name="gather",
    )(mix_share, *(pltpu.with_memory_space_constraint(w, pltpu.HBM) for w in held))
    serve_gate, serve_up, scale_gate, scale_up, serve_router = pl.pallas_call(
        place_kernel,
        out_shape=(
            jax.ShapeDtypeStruct((1, n * share, width), jnp.bfloat16),
            jax.ShapeDtypeStruct((1, n * share, width), jnp.bfloat16),
            jax.ShapeDtypeStruct((1, width), jnp.float32),
            jax.ShapeDtypeStruct((1, width), jnp.float32),
            jax.ShapeDtypeStruct((owners, n * share), jnp.bfloat16),
        ),
        in_specs=[in_vmem] * 3,
        out_specs=(in_hbm,) * 5,
        scratch_shapes=[pltpu.SemaphoreType.DMA((5,))],
        compiler_params=pltpu.CompilerParams(vmem_limit_bytes=32 * 2**20),
        name="place",
    )(gathered, scale, router)
    return (serve_gate, serve_up, scale_gate, scale_up, serve_router.T)


def solution(mesh):
    placed = (
        P("owner", "rows", None),
        P("owner", "rows", None),
        P("owner", "rows", None),
        P("owner", "rows", None),
        P("owner"),
        P("rows", "owner"),
        P("rows"),
    )
    return jax.shard_map(
        shards,
        mesh=mesh,
        in_specs=placed,
        out_specs=(
            P("owner", None, None),
            P("owner", None, None),
            P("owner", None),
            P("owner", None),
            P(),
        ),
        check_vma=False,
    )
```

```python
import functools

import jax
import jax.numpy as jnp
from jax import lax
from jax.experimental import pallas as pl
from jax.experimental.pallas import tpu as pltpu
from jax.sharding import PartitionSpec as P

SIDE = 4
STEP = 16
TALL, WIDE, CORES = 8, 4, 2
BEHIND = 16
APART = 7
GROUP = 3
SPREAD = 172.0
ACROSS = 9


def chunk_at(k, first):
    held = ACROSS if first else 16 - ACROSS
    return k // held, k % held + (0 if first else ACROSS)


def gather_kernel(
    mix, w_gate, avg_gate, w_up, avg_up, weight, gain,
    out, scale, router,
    coded, fresh, other, stats, factor, line, land, block,
    load, sent, stat_sent, stat_got, got,
    line_sent, line_got, z_sent, z_got, wide_sent, wide_got, core_sent, core_got,
):
    me = lax.axis_index("rows")
    owner = lax.axis_index("owner")
    high, y, core = owner // (WIDE * CORES), owner // CORES % WIDE, owner % CORES
    x, z = me % SIDE, me // SIDE
    right, left = z * SIDE + (x + 1) % SIDE, z * SIDE + (x + SIDE - 1) % SIDE
    across = (1 - z) * SIDE + x
    far = z * SIDE + (x + 2) % SIDE
    share = fresh.shape[1]
    n_first, n_rest = 2 * ACROSS, 2 * (16 - ACROSS)

    def at_owner(h, j, c):
        return {"owner": (h * WIDE + j) * CORES + c}

    loads = []
    for i, (source, target) in enumerate(
        (
            (w_gate.at[0], fresh.at[0]),
            (avg_gate.at[0], other.at[0]),
            (w_up.at[0], fresh.at[1]),
            (avg_up.at[0], other.at[1]),
            (weight, line.at[0]),
            (gain, line.at[1]),
        )
    ):
        loads.append(pltpu.make_async_copy(source, target, load.at[i]))
        loads[-1].start()

    barrier = pltpu.get_barrier_semaphore()
    for hop in range(1, 2 * SIDE):
        pl.semaphore_signal(barrier, inc=1, device_id={"rows": (me + hop) % (2 * SIDE)}, device_id_type=pl.DeviceIdType.MESH)

    onward = 2 * z - 1
    for there, step, row in ((high < TALL - 1, 1, x), (high > 0, -1, SIDE + x)):

        @pl.when(there)
        def _():
            target = at_owner(high + step, y, core) | {"rows": row}
            pl.semaphore_signal(barrier, inc=1, device_id=target, device_id_type=pl.DeviceIdType.MESH)

    others = [at_owner(high, (y + hop) % WIDE, core) for hop in range(1, WIDE)]
    others.append(at_owner(high, y, 1 - core))
    for target in others:
        pl.semaphore_signal(barrier, inc=1, device_id=target, device_id_type=pl.DeviceIdType.MESH)

    part = mix[0]

    def sums(a):
        loads[2 * a].wait()
        loads[2 * a + 1].wait()

        def mixed(i, total):
            rows = pl.ds(pl.multiple_of(i * 8, 8), 8)
            value = part * fresh[a, rows, :] + (1.0 - part) * other[a, rows, :]
            fresh[a, rows, :] = value
            return total + value * value

        total = lax.fori_loop(0, share // 8, mixed, jnp.zeros((8, fresh.shape[2]), jnp.float32), unroll=4)
        total = jnp.sum(total, axis=0, keepdims=True)
        stats[me, pl.ds(a, 1), :] = total
        return jnp.where(total > 0.0, 1.0 / jnp.sqrt(total), 0.0)

    over = [sums(0)]
    loads[4].wait()
    loads[5].wait()
    lanes = pl.ds(pl.multiple_of(me * share, share), share)
    land[high, y, core, :, lanes] = (line[0] * line[1]).astype(jnp.bfloat16).astype(jnp.float32)

    has_next = (high + onward >= 0) & (high + onward < TALL)
    greeted = 2 * SIDE - 1 + len(others) + 2 * has_next.astype(jnp.int32)
    pl.semaphore_wait(barrier, greeted)

    def stat_copy(hop):
        return pltpu.make_async_remote_copy(
            src_ref=stats.at[me],
            dst_ref=stats.at[me],
            send_sem=stat_sent.at[0],
            recv_sem=stat_got.at[0],
            device_id={"rows": (me + hop) % (2 * SIDE)},
            device_id_type=pl.DeviceIdType.MESH,
        )

    def remote(place, send_sem, recv_sem, target):
        return pltpu.make_async_remote_copy(
            src_ref=place,
            dst_ref=place,
            send_sem=send_sem,
            recv_sem=recv_sem,
            device_id=target,
            device_id_type=pl.DeviceIdType.MESH,
        )

    def line_place(source):
        return land.at[high, y, core, :, pl.ds(pl.multiple_of(source * share, share), share)]

    def line_copy(hop):
        return remote(line_place(me), line_sent.at[0], line_got.at[0], {"rows": (me + hop) % (2 * SIDE)})

    def z_copy(row, step):
        target = at_owner(high + onward, y, core) | {"rows": (me, across)[row]}
        return remote(land.at[high - onward * step, y, core], z_sent.at[step], z_got.at[1 - z, step], target)

    def z_sends(step):
        behind = high - onward * step
        return has_next & (behind >= 0) & (behind < TALL)

    def z_comes(way, step):
        return (high >= step + 1) if way == 0 else (high + step + 1 <= TALL - 1)

    def z_step(step):
        if step > 0:
            for way in range(2):

                @pl.when(z_comes(way, step - 1))
                def _():
                    tile = land.at[high - (1 - 2 * way) * step, y, core]
                    pltpu.make_async_copy(tile, tile, z_got.at[way, step - 1]).wait()

        if step < TALL - 1:

            @pl.when(z_sends(step))
            def _():
                for row in range(2):
                    z_copy(row, step).start()

    def wide_copy(hop):
        target = at_owner(high, (y + hop) % WIDE, core)
        return remote(land.at[:, y, core], wide_sent.at[0], wide_got.at[0], target)

    def core_copy():
        return remote(land.at[:, :, core], core_sent.at[0], core_got.at[0], at_owner(high, y, 1 - core))

    def local_wait(place, sem):
        pltpu.make_async_copy(place, place, sem).wait()

    all_stats = stats.at[pl.ds(0, 2 * SIDE - 1)]
    all_lines = land.at[0, 0, 0, :, pl.ds(0, (2 * SIDE - 1) * share)]
    all_wide = land.at[:, pl.ds(0, WIDE - 1), 0]
    for hop in range(1, 2 * SIDE):
        line_copy(hop).start()
    def norms():
        local_wait(all_stats, stat_got.at[0])
        total = stats[0]
        for source in range(1, 2 * SIDE):
            total = total + stats[source]
        scale[...] = jnp.sqrt(total)
        for source in range(2 * SIDE):
            factor[source] = jnp.sqrt(stats[source]) / scale[...]

    def place(source, a, i):
        return coded.at[a, pl.ds(pl.multiple_of(source * share + i * STEP, STEP), STEP), :]

    def send(source, a, i, target, link, slot):
        pltpu.make_async_remote_copy(
            src_ref=place(source, a, i),
            dst_ref=place(source, a, i),
            send_sem=sent.at[link],
            recv_sem=got.at[link, slot // GROUP],
            device_id={"rows": target},
            device_id_type=pl.DeviceIdType.MESH,
        ).start()

    def rows_of(source, i):
        return pl.ds(pl.multiple_of(source * share + i * STEP, STEP), STEP)

    def encode(a, i):
        value = fresh[a, pl.ds(i * STEP, STEP), :]
        size = jnp.exp(SPREAD * jnp.sqrt(jnp.abs(value) * over[a]) - 0.5 * SPREAD)
        coded[a, rows_of(me, i), :] = jnp.where(value < 0.0, -size, size).astype(jnp.bfloat16)

    def decode(source, a, i):
        code = coded[a, rows_of(source, i), :].astype(jnp.float32)
        root = jnp.log(jnp.abs(code)) * (1.0 / SPREAD) + 0.5
        size = root * root * factor[source, pl.ds(a, 1), :]
        out[a, rows_of(source, i), :] = jnp.where(code < 0.0, -size, size).astype(jnp.bfloat16)

    def settle(k, _):
        a, i = k // 16, k % 16
        value = fresh[a, rows_of(0, i), :] / scale[pl.ds(a, 1), :]
        out[a, rows_of(me, i), :] = value.astype(jnp.bfloat16)
        return 0

    def flip(r):
        return (r + SIDE) % (2 * SIDE)

    firsts = [(True, k) for k in range(n_first)]
    rests = [(False, k) for k in range(n_rest)]

    def round_x(near, way):
        return (
            [(me, c) for c in rests]
            + [(me, c) for c in firsts]
            + [(near, c) for c in rests[way::2]]
            + [(across, c) for c in firsts]
            + [(near, c) for c in firsts[way::2]]
            + [(flip(near), c) for c in firsts[way::2]]
        )

    def from_x(near, way):
        return (
            (near, rests),
            (near, firsts),
            (far, rests[way::2]),
            (flip(near), firsts),
            (far, firsts[way::2]),
            (flip(far), firsts[way::2]),
        )

    def over_z(own, one, two, three):
        return ((own, firsts), (own, rests), (one, rests), (two, rests), (three, rests))

    goes = (
        round_x(left, 0),
        round_x(right, 1),
        [(source, c) for source, run in over_z(me, left, right, far) for c in run],
    )
    runs = (from_x(left, 0), from_x(right, 1), over_z(across, flip(left), flip(right), flip(far)))
    comes = tuple([(source, run, at) for source, run in each for at in range(len(run))] for each in runs)

    def decode_run(source, run, begin, end):
        first, k = run[begin]
        stride = run[1][1] - run[0][1]

        def one(j, _):
            decode(source, *chunk_at(k + stride * j, first))
            return 0

        lax.fori_loop(0, end - begin, one, 0)

    targets = (right, left, across)
    slots = max(len(g) for g in goes)

    def line_wait():
        local_wait(all_lines, line_got.at[0])

    def wide_wait():
        local_wait(all_wide, wide_got.at[0])

    def router_step(step):
        if step == 0:
            line_wait()
        if step < TALL:
            z_step(step)
        if step == TALL - 1:
            for hop in range(1, WIDE):
                wide_copy(hop).start()
        if step == TALL:
            wide_wait()
            core_copy().start()
        if step == TALL + 1:
            theirs = land.at[:, :, 1 - core]
            pltpu.make_async_copy(theirs, theirs, core_got.at[0]).wait()
            for first in range(0, TALL * WIDE * CORES, 16):

                def line_in(k, _):
                    o = first + k
                    block[pl.ds(k, 1), :] = land[o // (WIDE * CORES), o // CORES % WIDE, o % CORES]
                    return 0

                lax.fori_loop(0, 16, line_in, 0)
                router[pl.ds(first, 16), :] = block[...].astype(jnp.bfloat16)

    def encode_pair(k):
        for chunks in (firsts, rests):
            if k < len(chunks):
                first, at = chunks[k]
                encode(*chunk_at(at, first))

    encode_pair(0)
    waiting = [0, 0, 0]
    for slot in range(slots + BEHIND):
        if slot == 3:
            over.append(sums(1))
            for hop in range(1, 2 * SIDE):
                stat_copy(hop).start()
        encode_pair(slot + 1)
        if slot == BEHIND - 1:
            norms()
        if slot in range(BEHIND + 3, BEHIND + 19, 2):
            begin = (slot - BEHIND - 3) * 2
            lax.fori_loop(begin, begin + 4, settle, 0)
        for link in range(3):
            at = slot - BEHIND
            if not 0 <= at < len(comes[link]) or (at % GROUP < GROUP - 1 and at < len(comes[link]) - 1):
                continue
            group = comes[link][at // GROUP * GROUP : at + 1]
            local_wait(coded.at[0, pl.ds(0, len(group) * STEP), :], got.at[link, at // GROUP])
            for source, run, j in group:
                waiting[link] += 1
                if waiting[link] == 6 or j == len(run) - 1 or at >= slots - 6:
                    decode_run(source, run, j + 1 - waiting[link], j + 1)
                    waiting[link] = 0
        if slot % APART == APART // 2 and slot // APART <= TALL + 1:
            router_step(slot // APART)
        for link in range(3):
            if slot < len(goes[link]):
                source, (first, at) = goes[link][slot]
                send(source, *chunk_at(at, first), targets[link], link, slot)

    local_wait(all_stats, stat_sent.at[0])
    local_wait(all_lines, line_sent.at[0])
    local_wait(all_wide, wide_sent.at[0])
    for step in range(TALL - 1):

        @pl.when(z_sends(step))
        def _():
            local_wait(land.at[pl.ds(0, 2), 0, 0], z_sent.at[step])

    core_copy().wait_send()
    for link in range(3):
        count = len(goes[link])
        all_sent = coded.at[0, pl.ds(0, count * STEP), :]
        pltpu.make_async_copy(all_sent, all_sent, sent.at[link]).wait()


def place_kernel(gathered, scale, router, serve_gate, serve_up, scale_gate, scale_up, serve_router, done):
    rows = gathered.shape[1] // 8
    copies = [
        pltpu.make_async_copy(scale.at[pl.ds(0, 1)], scale_gate, done.at[16]),
        pltpu.make_async_copy(scale.at[pl.ds(1, 1)], scale_up, done.at[17]),
        pltpu.make_async_copy(router, serve_router, done.at[18]),
    ]
    for a, target in enumerate((serve_gate, serve_up)):
        for p in range(8):
            piece = pl.ds(p * rows, rows)
            copies.append(pltpu.make_async_copy(gathered.at[a, piece], target.at[0, piece], done.at[a * 8 + p]))
    for copy in copies:
        copy.start()
    for copy in copies:
        copy.wait()


def shards(w_gate, avg_gate, w_up, avg_up, mix_share, router_weight, router_gain):
    _, share, width = w_gate.shape
    n = lax.axis_size("rows")
    in_hbm = pl.BlockSpec(memory_space=pltpu.HBM)
    in_vmem = pl.BlockSpec(memory_space=pltpu.VMEM)
    held = (w_gate, avg_gate, w_up, avg_up, router_weight.T, router_gain[None])
    owners = TALL * WIDE * CORES
    gathered, scale, router = pl.pallas_call(
        gather_kernel,
        out_shape=(
            jax.ShapeDtypeStruct((2, n * share, width), jnp.bfloat16),
            jax.ShapeDtypeStruct((2, width), jnp.float32),
            jax.ShapeDtypeStruct((owners, n * share), jnp.bfloat16),
        ),
        in_specs=[pl.BlockSpec(memory_space=pltpu.SMEM)] + [in_hbm] * 6,
        out_specs=(in_vmem,) * 3,
        scratch_shapes=[
            pltpu.VMEM((2, n * share, width), jnp.bfloat16),
            pltpu.VMEM((2, share, width), jnp.float32),
            pltpu.VMEM((2, share, width), jnp.float32),
            pltpu.VMEM((n, 2, width), jnp.float32),
            pltpu.VMEM((n, 2, width), jnp.float32),
            pltpu.VMEM((2, 1, share), jnp.float32),
            pltpu.VMEM((TALL, WIDE, CORES, 1, n * share), jnp.float32),
            pltpu.VMEM((16, n * share), jnp.float32),
            pltpu.SemaphoreType.DMA((6,)),
            pltpu.SemaphoreType.DMA((3,)),
            pltpu.SemaphoreType.DMA((1,)),
            pltpu.SemaphoreType.DMA((1,)),
            pltpu.SemaphoreType.DMA((3, 25)),
            pltpu.SemaphoreType.DMA((1,)),
            pltpu.SemaphoreType.DMA((1,)),
            pltpu.SemaphoreType.DMA((TALL - 1,)),
            pltpu.SemaphoreType.DMA((2, TALL - 1)),
            pltpu.SemaphoreType.DMA((1,)),
            pltpu.SemaphoreType.DMA((1,)),
            pltpu.SemaphoreType.DMA((1,)),
            pltpu.SemaphoreType.DMA((1,)),
        ],
        compiler_params=pltpu.CompilerParams(collective_id=0, has_side_effects=True, vmem_limit_bytes=32 * 2**20),
        name="gather",
    )(mix_share, *(pltpu.with_memory_space_constraint(w, pltpu.HBM) for w in held))
    serve_gate, serve_up, scale_gate, scale_up, serve_router = pl.pallas_call(
        place_kernel,
        out_shape=(
            jax.ShapeDtypeStruct((1, n * share, width), jnp.bfloat16),
            jax.ShapeDtypeStruct((1, n * share, width), jnp.bfloat16),
            jax.ShapeDtypeStruct((1, width), jnp.float32),
            jax.ShapeDtypeStruct((1, width), jnp.float32),
            jax.ShapeDtypeStruct((owners, n * share), jnp.bfloat16),
        ),
        in_specs=[in_vmem] * 3,
        out_specs=(in_hbm,) * 5,
        scratch_shapes=[pltpu.SemaphoreType.DMA((19,))],
        compiler_params=pltpu.CompilerParams(vmem_limit_bytes=32 * 2**20),
        name="place",
    )(gathered, scale, router)
    return (serve_gate, serve_up, scale_gate, scale_up, serve_router.T)


def solution(mesh):
    placed = (
        P("owner", "rows", None),
        P("owner", "rows", None),
        P("owner", "rows", None),
        P("owner", "rows", None),
        P("owner"),
        P("rows", "owner"),
        P("rows"),
    )
    return jax.shard_map(
        shards,
        mesh=mesh,
        in_specs=placed,
        out_specs=(
            P("owner", None, None),
            P("owner", None, None),
            P("owner", None),
            P("owner", None),
            P(),
        ),
        check_vma=False,
    )
```

```python
import functools

import jax
import jax.numpy as jnp
from jax import lax
from jax.experimental import pallas as pl
from jax.experimental.pallas import tpu as pltpu
from jax.sharding import PartitionSpec as P

SIDE = 4
STEP = 16
TALL, WIDE, CORES = 8, 4, 2
BEHIND = 15
APART = 7
GROUP = 4
SPREAD = 172.0
ACROSS = 9


def chunk_at(k, first):
    held = ACROSS if first else 16 - ACROSS
    return k // held, k % held + (0 if first else ACROSS)


def gather_kernel(
    mix, w_gate, avg_gate, w_up, avg_up, weight, gain,
    out, scale, router,
    coded, fresh, other, stats, factor, line, land, block,
    load, sent, stat_sent, stat_got, got,
    line_sent, line_got, z_sent, z_got, wide_sent, wide_got, core_sent, core_got,
):
    me = lax.axis_index("rows")
    owner = lax.axis_index("owner")
    high, y, core = owner // (WIDE * CORES), owner // CORES % WIDE, owner % CORES
    x, z = me % SIDE, me // SIDE
    right, left = z * SIDE + (x + 1) % SIDE, z * SIDE + (x + SIDE - 1) % SIDE
    across = (1 - z) * SIDE + x
    far = z * SIDE + (x + 2) % SIDE
    share = fresh.shape[1]
    n_first, n_rest = 2 * ACROSS, 2 * (16 - ACROSS)

    def at_owner(h, j, c):
        return {"owner": (h * WIDE + j) * CORES + c}

    loads = []
    for i, (source, target) in enumerate(
        (
            (w_gate.at[0], fresh.at[0]),
            (avg_gate.at[0], other.at[0]),
            (w_up.at[0], fresh.at[1]),
            (avg_up.at[0], other.at[1]),
            (weight, line.at[0]),
            (gain, line.at[1]),
        )
    ):
        loads.append(pltpu.make_async_copy(source, target, load.at[i]))
    for i in (0, 1, 4, 5):
        loads[i].start()

    barrier = pltpu.get_barrier_semaphore()
    for hop in range(1, 2 * SIDE):
        pl.semaphore_signal(barrier, inc=1, device_id={"rows": (me + hop) % (2 * SIDE)}, device_id_type=pl.DeviceIdType.MESH)

    onward = 2 * z - 1
    for there, step, row in ((high < TALL - 1, 1, x), (high > 0, -1, SIDE + x)):

        @pl.when(there)
        def _():
            target = at_owner(high + step, y, core) | {"rows": row}
            pl.semaphore_signal(barrier, inc=1, device_id=target, device_id_type=pl.DeviceIdType.MESH)

    others = [at_owner(high, (y + hop) % WIDE, core) for hop in range(1, WIDE)]
    others.append(at_owner(high, y, 1 - core))
    for target in others:
        pl.semaphore_signal(barrier, inc=1, device_id=target, device_id_type=pl.DeviceIdType.MESH)


    def sums(a):
        loads[2 * a].wait()
        loads[2 * a + 1].wait()
        if a == 0:
            loads[2].start()
            loads[3].start()
        part = mix[0]

        def mixed(i, total):
            rows = pl.ds(pl.multiple_of(i * 8, 8), 8)
            value = part * fresh[a, rows, :] + (1.0 - part) * other[a, rows, :]
            fresh[a, rows, :] = value
            return total + value * value

        total = lax.fori_loop(0, share // 8, mixed, jnp.zeros((8, fresh.shape[2]), jnp.float32), unroll=4)
        total = jnp.sum(total, axis=0, keepdims=True)
        stats[me, pl.ds(a, 1), :] = total
        return jnp.where(total > 0.0, 1.0 / jnp.sqrt(total), 0.0)

    over = [sums(0)]
    loads[4].wait()
    loads[5].wait()
    lanes = pl.ds(pl.multiple_of(me * share, share), share)
    land[high, y, core, :, lanes] = (line[0] * line[1]).astype(jnp.bfloat16).astype(jnp.float32)

    has_next = (high + onward >= 0) & (high + onward < TALL)
    greeted = 2 * SIDE - 1 + len(others) + 2 * has_next.astype(jnp.int32)

    def stat_copy(hop):
        return pltpu.make_async_remote_copy(
            src_ref=stats.at[me],
            dst_ref=stats.at[me],
            send_sem=stat_sent.at[0],
            recv_sem=stat_got.at[0],
            device_id={"rows": (me + hop) % (2 * SIDE)},
            device_id_type=pl.DeviceIdType.MESH,
        )

    def remote(place, send_sem, recv_sem, target):
        return pltpu.make_async_remote_copy(
            src_ref=place,
            dst_ref=place,
            send_sem=send_sem,
            recv_sem=recv_sem,
            device_id=target,
            device_id_type=pl.DeviceIdType.MESH,
        )

    def line_place(source):
        return land.at[high, y, core, :, pl.ds(pl.multiple_of(source * share, share), share)]

    def line_copy(hop):
        return remote(line_place(me), line_sent.at[0], line_got.at[0], {"rows": (me + hop) % (2 * SIDE)})

    def z_copy(row, step):
        target = at_owner(high + onward, y, core) | {"rows": (me, across)[row]}
        return remote(land.at[high - onward * step, y, core], z_sent.at[step], z_got.at[1 - z, step], target)

    def z_sends(step):
        behind = high - onward * step
        return has_next & (behind >= 0) & (behind < TALL)

    def z_comes(way, step):
        return (high >= step + 1) if way == 0 else (high + step + 1 <= TALL - 1)

    def z_step(step):
        if step > 0:
            for way in range(2):

                @pl.when(z_comes(way, step - 1))
                def _():
                    tile = land.at[high - (1 - 2 * way) * step, y, core]
                    pltpu.make_async_copy(tile, tile, z_got.at[way, step - 1]).wait()

        if step < TALL - 1:

            @pl.when(z_sends(step))
            def _():
                for row in range(2):
                    z_copy(row, step).start()

    def wide_copy(hop):
        target = at_owner(high, (y + hop) % WIDE, core)
        return remote(land.at[:, y, core], wide_sent.at[0], wide_got.at[0], target)

    def core_copy():
        return remote(land.at[:, :, core], core_sent.at[0], core_got.at[0], at_owner(high, y, 1 - core))

    def local_wait(place, sem):
        pltpu.make_async_copy(place, place, sem).wait()

    all_stats = stats.at[pl.ds(0, 2 * SIDE - 1)]
    all_lines = land.at[0, 0, 0, :, pl.ds(0, (2 * SIDE - 1) * share)]
    all_wide = land.at[:, pl.ds(0, WIDE - 1), 0]
    def norms():
        local_wait(all_stats, stat_got.at[0])
        total = stats[0]
        for source in range(1, 2 * SIDE):
            total = total + stats[source]
        scale[...] = jnp.sqrt(total)
        for source in range(2 * SIDE):
            factor[source] = jnp.sqrt(stats[source]) / scale[...]

    def place(source, a, i):
        return coded.at[a, pl.ds(pl.multiple_of(source * share + i * STEP, STEP), STEP), :]

    def send(source, a, i, target, link, slot):
        pltpu.make_async_remote_copy(
            src_ref=place(source, a, i),
            dst_ref=place(source, a, i),
            send_sem=sent.at[link],
            recv_sem=got.at[link, slot // GROUP],
            device_id={"rows": target},
            device_id_type=pl.DeviceIdType.MESH,
        ).start()

    def rows_of(source, i):
        return pl.ds(pl.multiple_of(source * share + i * STEP, STEP), STEP)

    def encode(a, i):
        value = fresh[a, pl.ds(i * STEP, STEP), :]
        size = jnp.exp(SPREAD * jnp.sqrt(jnp.abs(value) * over[a]) - 0.5 * SPREAD)
        coded[a, rows_of(me, i), :] = jnp.where(value < 0.0, -size, size).astype(jnp.bfloat16)

    def decode(source, a, i):
        code = coded[a, rows_of(source, i), :].astype(jnp.float32)
        root = jnp.log(jnp.abs(code)) * (1.0 / SPREAD) + 0.5
        size = root * root * factor[source, pl.ds(a, 1), :]
        out[a, rows_of(source, i), :] = jnp.where(code < 0.0, -size, size).astype(jnp.bfloat16)

    def settle(k, _):
        a, i = k // 16, k % 16
        value = fresh[a, rows_of(0, i), :] / scale[pl.ds(a, 1), :]
        out[a, rows_of(me, i), :] = value.astype(jnp.bfloat16)
        return 0

    def flip(r):
        return (r + SIDE) % (2 * SIDE)

    firsts = [(True, k) for k in range(n_first)]
    rests = [(False, k) for k in range(n_rest)]

    def round_x(near, way):
        return (
            [(me, c) for c in rests]
            + [(me, c) for c in firsts]
            + [(near, c) for c in rests[way::2]]
            + [(across, c) for c in firsts]
            + [(near, c) for c in firsts[way::2]]
            + [(flip(near), c) for c in firsts[way::2]]
        )

    def from_x(near, way):
        return (
            (near, rests),
            (near, firsts),
            (far, rests[way::2]),
            (flip(near), firsts),
            (far, firsts[way::2]),
            (flip(far), firsts[way::2]),
        )

    def over_z(own, one, two, three):
        return ((own, firsts), (own, rests), (one, rests), (two, rests), (three, rests))

    goes = (
        round_x(left, 0),
        round_x(right, 1),
        [(source, c) for source, run in over_z(me, left, right, far) for c in run],
    )
    runs = (from_x(left, 0), from_x(right, 1), over_z(across, flip(left), flip(right), flip(far)))
    comes = tuple([(source, run, at) for source, run in each for at in range(len(run))] for each in runs)

    def decode_run(source, run, begin, end):
        first, k = run[begin]
        stride = run[1][1] - run[0][1]

        def one(j, _):
            decode(source, *chunk_at(k + stride * j, first))
            return 0

        lax.fori_loop(0, end - begin, one, 0)

    targets = (right, left, across)
    slots = max(len(g) for g in goes)

    def line_wait():
        local_wait(all_lines, line_got.at[0])

    def wide_wait():
        local_wait(all_wide, wide_got.at[0])

    def router_step(step):
        if step == 0:
            line_wait()
        if step < TALL:
            z_step(step)
        if step == TALL - 1:
            for hop in range(1, WIDE):
                wide_copy(hop).start()
        if step == TALL:
            wide_wait()
            core_copy().start()
        if step == TALL + 1:
            theirs = land.at[:, :, 1 - core]
            pltpu.make_async_copy(theirs, theirs, core_got.at[0]).wait()
            for first in range(0, TALL * WIDE * CORES, 16):

                def line_in(k, _):
                    o = first + k
                    block[pl.ds(k, 1), :] = land[o // (WIDE * CORES), o // CORES % WIDE, o % CORES]
                    return 0

                lax.fori_loop(0, 16, line_in, 0)
                router[pl.ds(first, 16), :] = block[...].astype(jnp.bfloat16)

    def encode_pair(k):
        for chunks in (firsts, rests):
            if k < len(chunks):
                first, at = chunks[k]
                encode(*chunk_at(at, first))

    for k in range(3):
        encode_pair(k)
    pl.semaphore_wait(barrier, greeted)
    for hop in range(1, 2 * SIDE):
        line_copy(hop).start()
    waiting = [0, 0, 0]
    for slot in range(slots + BEHIND):
        if slot == 3:
            over.append(sums(1))
            for hop in range(1, 2 * SIDE):
                stat_copy(hop).start()
        encode_pair(slot + 3)
        if slot == BEHIND - 1:
            norms()
        if slot in range(BEHIND + 3, BEHIND + 19, 2):
            begin = (slot - BEHIND - 3) * 2
            lax.fori_loop(begin, begin + 4, settle, 0)
        for link in range(3):
            at = slot - BEHIND
            if not 0 <= at < len(comes[link]) or (at % GROUP < GROUP - 1 and at < len(comes[link]) - 1):
                continue
            group = comes[link][at // GROUP * GROUP : at + 1]
            local_wait(coded.at[0, pl.ds(0, len(group) * STEP), :], got.at[link, at // GROUP])
            for source, run, j in group:
                waiting[link] += 1
                if waiting[link] == 6 or j == len(run) - 1 or at >= slots - 6:
                    decode_run(source, run, j + 1 - waiting[link], j + 1)
                    waiting[link] = 0
        if slot % APART == APART // 2 and 1 <= slot // APART <= TALL + 2:
            router_step(slot // APART - 1)
        for link in range(3):
            if slot < len(goes[link]):
                source, (first, at) = goes[link][slot]
                send(source, *chunk_at(at, first), targets[link], link, slot)

    local_wait(all_stats, stat_sent.at[0])
    local_wait(all_lines, line_sent.at[0])
    local_wait(all_wide, wide_sent.at[0])
    for step in range(TALL - 1):

        @pl.when(z_sends(step))
        def _():
            local_wait(land.at[pl.ds(0, 2), 0, 0], z_sent.at[step])

    core_copy().wait_send()
    for link in range(3):
        count = len(goes[link])
        all_sent = coded.at[0, pl.ds(0, count * STEP), :]
        pltpu.make_async_copy(all_sent, all_sent, sent.at[link]).wait()


def place_kernel(gathered, scale, router, serve_gate, serve_up, scale_gate, scale_up, serve_router, done):
    copies = (
        pltpu.make_async_copy(gathered.at[pl.ds(0, 1)], serve_gate, done.at[0]),
        pltpu.make_async_copy(gathered.at[pl.ds(1, 1)], serve_up, done.at[1]),
        pltpu.make_async_copy(scale.at[pl.ds(0, 1)], scale_gate, done.at[2]),
        pltpu.make_async_copy(scale.at[pl.ds(1, 1)], scale_up, done.at[3]),
        pltpu.make_async_copy(router, serve_router, done.at[4]),
    )
    for copy in copies:
        copy.start()
    for copy in copies:
        copy.wait()


def shards(w_gate, avg_gate, w_up, avg_up, mix_share, router_weight, router_gain):
    _, share, width = w_gate.shape
    n = lax.axis_size("rows")
    in_hbm = pl.BlockSpec(memory_space=pltpu.HBM)
    in_vmem = pl.BlockSpec(memory_space=pltpu.VMEM)
    held = (w_gate, avg_gate, w_up, avg_up, router_weight.T, router_gain[None])
    owners = TALL * WIDE * CORES
    gathered, scale, router = pl.pallas_call(
        gather_kernel,
        out_shape=(
            jax.ShapeDtypeStruct((2, n * share, width), jnp.bfloat16),
            jax.ShapeDtypeStruct((2, width), jnp.float32),
            jax.ShapeDtypeStruct((owners, n * share), jnp.bfloat16),
        ),
        in_specs=[pl.BlockSpec(memory_space=pltpu.SMEM)] + [in_hbm] * 6,
        out_specs=(in_vmem,) * 3,
        scratch_shapes=[
            pltpu.VMEM((2, n * share, width), jnp.bfloat16),
            pltpu.VMEM((2, share, width), jnp.float32),
            pltpu.VMEM((2, share, width), jnp.float32),
            pltpu.VMEM((n, 2, width), jnp.float32),
            pltpu.VMEM((n, 2, width), jnp.float32),
            pltpu.VMEM((2, 1, share), jnp.float32),
            pltpu.VMEM((TALL, WIDE, CORES, 1, n * share), jnp.float32),
            pltpu.VMEM((16, n * share), jnp.float32),
            pltpu.SemaphoreType.DMA((6,)),
            pltpu.SemaphoreType.DMA((3,)),
            pltpu.SemaphoreType.DMA((1,)),
            pltpu.SemaphoreType.DMA((1,)),
            pltpu.SemaphoreType.DMA((3, 19)),
            pltpu.SemaphoreType.DMA((1,)),
            pltpu.SemaphoreType.DMA((1,)),
            pltpu.SemaphoreType.DMA((TALL - 1,)),
            pltpu.SemaphoreType.DMA((2, TALL - 1)),
            pltpu.SemaphoreType.DMA((1,)),
            pltpu.SemaphoreType.DMA((1,)),
            pltpu.SemaphoreType.DMA((1,)),
            pltpu.SemaphoreType.DMA((1,)),
        ],
        compiler_params=pltpu.CompilerParams(collective_id=0, has_side_effects=True, vmem_limit_bytes=32 * 2**20),
        name="gather",
    )(mix_share, *(pltpu.with_memory_space_constraint(w, pltpu.HBM) for w in held))
    serve_gate, serve_up, scale_gate, scale_up, serve_router = pl.pallas_call(
        place_kernel,
        out_shape=(
            jax.ShapeDtypeStruct((1, n * share, width), jnp.bfloat16),
            jax.ShapeDtypeStruct((1, n * share, width), jnp.bfloat16),
            jax.ShapeDtypeStruct((1, width), jnp.float32),
            jax.ShapeDtypeStruct((1, width), jnp.float32),
            jax.ShapeDtypeStruct((owners, n * share), jnp.bfloat16),
        ),
        in_specs=[in_vmem] * 3,
        out_specs=(in_hbm,) * 5,
        scratch_shapes=[pltpu.SemaphoreType.DMA((5,))],
        compiler_params=pltpu.CompilerParams(vmem_limit_bytes=32 * 2**20),
        name="place",
    )(gathered, scale, router)
    return (serve_gate, serve_up, scale_gate, scale_up, serve_router.T)


def solution(mesh):
    placed = (
        P("owner", "rows", None),
        P("owner", "rows", None),
        P("owner", "rows", None),
        P("owner", "rows", None),
        P("owner"),
        P("rows", "owner"),
        P("rows"),
    )
    return jax.shard_map(
        shards,
        mesh=mesh,
        in_specs=placed,
        out_specs=(
            P("owner", None, None),
            P("owner", None, None),
            P("owner", None),
            P("owner", None),
            P(),
        ),
        check_vma=False,
    )
```

```python
import functools

import jax
import jax.numpy as jnp
from jax import lax
from jax.experimental import pallas as pl
from jax.experimental.pallas import tpu as pltpu
from jax.sharding import PartitionSpec as P

SIDE = 4
STEP = 16
TALL, WIDE, CORES = 8, 4, 2
BEHIND = 15
APART = 7
GROUP = 4
SPREAD = 172.0
ACROSS = 9


def chunk_at(k, first):
    held = ACROSS if first else 16 - ACROSS
    return k // held, k % held + (0 if first else ACROSS)


def gather_kernel(
    mix, w_gate, avg_gate, w_up, avg_up, weight, gain,
    out, scale, router,
    coded, fresh, other, stats, factor, line, land, block,
    load, sent, stat_sent, stat_got, got,
    line_sent, line_got, z_sent, z_got, wide_sent, wide_got, core_sent, core_got, above_in,
):
    me = lax.axis_index("rows")
    owner = lax.axis_index("owner")
    high, y, core = owner // (WIDE * CORES), owner // CORES % WIDE, owner % CORES
    x, z = me % SIDE, me // SIDE
    right, left = z * SIDE + (x + 1) % SIDE, z * SIDE + (x + SIDE - 1) % SIDE
    across = (1 - z) * SIDE + x
    far = z * SIDE + (x + 2) % SIDE
    share = fresh.shape[1]
    n_first, n_rest = 2 * ACROSS, 2 * (16 - ACROSS)

    def at_owner(h, j, c):
        return {"owner": (h * WIDE + j) * CORES + c}

    loads = []
    for i, (source, target) in enumerate(
        (
            (w_gate.at[0], fresh.at[0]),
            (avg_gate.at[0], other.at[0]),
            (w_up.at[0], fresh.at[1]),
            (avg_up.at[0], other.at[1]),
            (weight, line.at[0]),
            (gain, line.at[1]),
        )
    ):
        loads.append(pltpu.make_async_copy(source, target, load.at[i]))
    for i in (0, 1, 4, 5):
        loads[i].start()

    barrier = pltpu.get_barrier_semaphore()
    for hop in range(1, 2 * SIDE):
        pl.semaphore_signal(barrier, inc=1, device_id={"rows": (me + hop) % (2 * SIDE)}, device_id_type=pl.DeviceIdType.MESH)

    onward = 2 * z - 1

    @pl.when(high < TALL - 1)
    def _():
        target = at_owner(high + 1, y, core) | {"rows": x}
        pl.semaphore_signal(barrier, inc=1, device_id=target, device_id_type=pl.DeviceIdType.MESH)

    others = [at_owner(high, (y + hop) % WIDE, core) for hop in range(1, WIDE)]
    others.append(at_owner(high, y, 1 - core))
    for target in others:
        pl.semaphore_signal(barrier, inc=1, device_id=target, device_id_type=pl.DeviceIdType.MESH)


    def sums(a):
        loads[2 * a].wait()
        loads[2 * a + 1].wait()
        if a == 0:
            loads[2].start()
            loads[3].start()
        part = mix[0]

        def mixed(i, total):
            rows = pl.ds(pl.multiple_of(i * 8, 8), 8)
            value = part * fresh[a, rows, :] + (1.0 - part) * other[a, rows, :]
            fresh[a, rows, :] = value
            return total + value * value

        total = lax.fori_loop(0, share // 8, mixed, jnp.zeros((8, fresh.shape[2]), jnp.float32), unroll=4)
        total = jnp.sum(total, axis=0, keepdims=True)
        stats[me, pl.ds(a, 1), :] = total
        return jnp.where(total > 0.0, 1.0 / jnp.sqrt(total), 0.0)

    over = [sums(0)]
    loads[4].wait()
    loads[5].wait()
    lanes = pl.ds(pl.multiple_of(me * share, share), share)
    land[high, y, core, :, lanes] = (line[0] * line[1]).astype(jnp.bfloat16).astype(jnp.float32)

    has_next = (high + onward >= 0) & (high + onward < TALL)
    sends_down, sends_up = (z == 0) & (high > 0), (z == 1) & (high < TALL - 1)
    greeted = 2 * SIDE - 1 + len(others) + 2 * sends_down.astype(jnp.int32)

    def stat_copy(hop):
        return pltpu.make_async_remote_copy(
            src_ref=stats.at[me],
            dst_ref=stats.at[me],
            send_sem=stat_sent.at[0],
            recv_sem=stat_got.at[0],
            device_id={"rows": (me + hop) % (2 * SIDE)},
            device_id_type=pl.DeviceIdType.MESH,
        )

    def remote(place, send_sem, recv_sem, target):
        return pltpu.make_async_remote_copy(
            src_ref=place,
            dst_ref=place,
            send_sem=send_sem,
            recv_sem=recv_sem,
            device_id=target,
            device_id_type=pl.DeviceIdType.MESH,
        )

    def line_place(source):
        return land.at[high, y, core, :, pl.ds(pl.multiple_of(source * share, share), share)]

    def line_copy(hop):
        return remote(line_place(me), line_sent.at[0], line_got.at[0], {"rows": (me + hop) % (2 * SIDE)})

    def z_copy(row, step):
        target = at_owner(high + onward, y, core) | {"rows": (me, across)[row]}
        return remote(land.at[high - onward * step, y, core], z_sent.at[step], z_got.at[1 - z, step], target)

    def z_sends(step):
        behind = high - onward * step
        return has_next & (behind >= 0) & (behind < TALL)

    def z_comes(way, step):
        return (high >= step + 1) if way == 0 else (high + step + 1 <= TALL - 1)

    def z_step(step):
        if step > 0:
            for way in range(2):

                @pl.when(z_comes(way, step - 1))
                def _():
                    tile = land.at[high - (1 - 2 * way) * step, y, core]
                    pltpu.make_async_copy(tile, tile, z_got.at[way, step - 1]).wait()

        if step < TALL - 1:

            @pl.when(z_sends(step))
            def _():
                for row in range(2):
                    z_copy(row, step).start()

    def wide_copy(hop):
        target = at_owner(high, (y + hop) % WIDE, core)
        return remote(land.at[:, y, core], wide_sent.at[0], wide_got.at[0], target)

    def core_copy():
        return remote(land.at[:, :, core], core_sent.at[0], core_got.at[0], at_owner(high, y, 1 - core))

    def local_wait(place, sem):
        pltpu.make_async_copy(place, place, sem).wait()

    all_stats = stats.at[pl.ds(0, 2 * SIDE - 1)]
    all_lines = land.at[0, 0, 0, :, pl.ds(0, (2 * SIDE - 1) * share)]
    all_wide = land.at[:, pl.ds(0, WIDE - 1), 0]
    def norms():
        local_wait(all_stats, stat_got.at[0])
        total = stats[0]
        for source in range(1, 2 * SIDE):
            total = total + stats[source]
        scale[...] = jnp.sqrt(total)
        for source in range(2 * SIDE):
            factor[source] = jnp.sqrt(stats[source]) / scale[...]

    def place(source, a, i):
        return coded.at[a, pl.ds(pl.multiple_of(source * share + i * STEP, STEP), STEP), :]

    def send(source, a, i, target, link, slot):
        pltpu.make_async_remote_copy(
            src_ref=place(source, a, i),
            dst_ref=place(source, a, i),
            send_sem=sent.at[link],
            recv_sem=got.at[link, slot // GROUP],
            device_id={"rows": target},
            device_id_type=pl.DeviceIdType.MESH,
        ).start()

    def rows_of(source, i):
        return pl.ds(pl.multiple_of(source * share + i * STEP, STEP), STEP)

    def encode(a, i):
        value = fresh[a, pl.ds(i * STEP, STEP), :]
        size = jnp.exp(SPREAD * jnp.sqrt(jnp.abs(value) * over[a]) - 0.5 * SPREAD)
        coded[a, rows_of(me, i), :] = jnp.where(value < 0.0, -size, size).astype(jnp.bfloat16)

    def decode(source, a, i):
        code = coded[a, rows_of(source, i), :].astype(jnp.float32)
        root = jnp.log(jnp.abs(code)) * (1.0 / SPREAD) + 0.5
        size = root * root * factor[source, pl.ds(a, 1), :]
        out[a, rows_of(source, i), :] = jnp.where(code < 0.0, -size, size).astype(jnp.bfloat16)

    def settle(k, _):
        a, i = k // 16, k % 16
        value = fresh[a, rows_of(0, i), :] / scale[pl.ds(a, 1), :]
        out[a, rows_of(me, i), :] = value.astype(jnp.bfloat16)
        return 0

    def flip(r):
        return (r + SIDE) % (2 * SIDE)

    firsts = [(True, k) for k in range(n_first)]
    rests = [(False, k) for k in range(n_rest)]

    def round_x(near, way):
        return (
            [(me, c) for c in rests]
            + [(me, c) for c in firsts]
            + [(near, c) for c in rests[way::2]]
            + [(across, c) for c in firsts]
            + [(near, c) for c in firsts[way::2]]
            + [(flip(near), c) for c in firsts[way::2]]
        )

    def from_x(near, way):
        return (
            (near, rests),
            (near, firsts),
            (far, rests[way::2]),
            (flip(near), firsts),
            (far, firsts[way::2]),
            (flip(far), firsts[way::2]),
        )

    def over_z(own, one, two, three):
        return ((own, firsts), (own, rests), (one, rests), (two, rests), (three, rests))

    goes = (
        round_x(left, 0),
        round_x(right, 1),
        [(source, c) for source, run in over_z(me, left, right, far) for c in run],
    )
    runs = (from_x(left, 0), from_x(right, 1), over_z(across, flip(left), flip(right), flip(far)))
    comes = tuple([(source, run, at) for source, run in each for at in range(len(run))] for each in runs)

    def decode_run(source, run, begin, end):
        first, k = run[begin]
        stride = run[1][1] - run[0][1]

        def one(j, _):
            decode(source, *chunk_at(k + stride * j, first))
            return 0

        lax.fori_loop(0, end - begin, one, 0)

    targets = (right, left, across)
    slots = max(len(g) for g in goes)

    def line_wait():
        local_wait(all_lines, line_got.at[0])

    def wide_wait():
        local_wait(all_wide, wide_got.at[0])

    def router_step(step):
        if step == 0:
            line_wait()

            @pl.when(sends_up)
            def _():
                pl.semaphore_wait(above_in, 1)

        if step < TALL:
            z_step(step)
        if step == TALL - 1:
            for hop in range(1, WIDE):
                wide_copy(hop).start()
        if step == TALL:
            wide_wait()
            core_copy().start()
        if step == TALL + 1:
            theirs = land.at[:, :, 1 - core]
            pltpu.make_async_copy(theirs, theirs, core_got.at[0]).wait()
            for first in range(0, TALL * WIDE * CORES, 16):

                def line_in(k, _):
                    o = first + k
                    block[pl.ds(k, 1), :] = land[o // (WIDE * CORES), o // CORES % WIDE, o % CORES]
                    return 0

                lax.fori_loop(0, 16, line_in, 0)
                router[pl.ds(first, 16), :] = block[...].astype(jnp.bfloat16)

    def encode_pair(k):
        for chunks in (firsts, rests):
            if k < len(chunks):
                first, at = chunks[k]
                encode(*chunk_at(at, first))

    for k in range(3):
        encode_pair(k)
    pl.semaphore_wait(barrier, greeted)

    @pl.when(sends_down)
    def _():
        target = at_owner(high - 1, y, core) | {"rows": SIDE + x}
        pl.semaphore_signal(above_in, inc=1, device_id=target, device_id_type=pl.DeviceIdType.MESH)

    for hop in range(1, 2 * SIDE):
        line_copy(hop).start()
    waiting = [0, 0, 0]
    for slot in range(slots + BEHIND):
        if slot == 3:
            over.append(sums(1))
            for hop in range(1, 2 * SIDE):
                stat_copy(hop).start()
        encode_pair(slot + 3)
        if slot == BEHIND - 1:
            norms()
        if slot in range(BEHIND + 3, BEHIND + 19, 2):
            begin = (slot - BEHIND - 3) * 2
            lax.fori_loop(begin, begin + 4, settle, 0)
        for link in range(3):
            at = slot - BEHIND
            if not 0 <= at < len(comes[link]) or (at % GROUP < GROUP - 1 and at < len(comes[link]) - 1):
                continue
            group = comes[link][at // GROUP * GROUP : at + 1]
            local_wait(coded.at[0, pl.ds(0, len(group) * STEP), :], got.at[link, at // GROUP])
            for source, run, j in group:
                waiting[link] += 1
                if waiting[link] == 6 or j == len(run) - 1 or at >= slots - 6:
                    decode_run(source, run, j + 1 - waiting[link], j + 1)
                    waiting[link] = 0
        if slot % APART == APART // 2 and 1 <= slot // APART <= TALL + 2:
            router_step(slot // APART - 1)
        for link in range(3):
            if slot < len(goes[link]):
                source, (first, at) = goes[link][slot]
                send(source, *chunk_at(at, first), targets[link], link, slot)

    local_wait(all_stats, stat_sent.at[0])
    local_wait(all_lines, line_sent.at[0])
    local_wait(all_wide, wide_sent.at[0])
    for step in range(TALL - 1):

        @pl.when(z_sends(step))
        def _():
            local_wait(land.at[pl.ds(0, 2), 0, 0], z_sent.at[step])

    core_copy().wait_send()
    for link in range(3):
        count = len(goes[link])
        all_sent = coded.at[0, pl.ds(0, count * STEP), :]
        pltpu.make_async_copy(all_sent, all_sent, sent.at[link]).wait()


def place_kernel(gathered, scale, router, serve_gate, serve_up, scale_gate, scale_up, serve_router, done):
    copies = (
        pltpu.make_async_copy(gathered.at[pl.ds(0, 1)], serve_gate, done.at[0]),
        pltpu.make_async_copy(gathered.at[pl.ds(1, 1)], serve_up, done.at[1]),
        pltpu.make_async_copy(scale.at[pl.ds(0, 1)], scale_gate, done.at[2]),
        pltpu.make_async_copy(scale.at[pl.ds(1, 1)], scale_up, done.at[3]),
        pltpu.make_async_copy(router, serve_router, done.at[4]),
    )
    for copy in copies:
        copy.start()
    for copy in copies:
        copy.wait()


def shards(w_gate, avg_gate, w_up, avg_up, mix_share, router_weight, router_gain):
    _, share, width = w_gate.shape
    n = lax.axis_size("rows")
    in_hbm = pl.BlockSpec(memory_space=pltpu.HBM)
    in_vmem = pl.BlockSpec(memory_space=pltpu.VMEM)
    held = (w_gate, avg_gate, w_up, avg_up, router_weight.T, router_gain[None])
    owners = TALL * WIDE * CORES
    gathered, scale, router = pl.pallas_call(
        gather_kernel,
        out_shape=(
            jax.ShapeDtypeStruct((2, n * share, width), jnp.bfloat16),
            jax.ShapeDtypeStruct((2, width), jnp.float32),
            jax.ShapeDtypeStruct((owners, n * share), jnp.bfloat16),
        ),
        in_specs=[pl.BlockSpec(memory_space=pltpu.SMEM)] + [in_hbm] * 6,
        out_specs=(in_vmem,) * 3,
        scratch_shapes=[
            pltpu.VMEM((2, n * share, width), jnp.bfloat16),
            pltpu.VMEM((2, share, width), jnp.float32),
            pltpu.VMEM((2, share, width), jnp.float32),
            pltpu.VMEM((n, 2, width), jnp.float32),
            pltpu.VMEM((n, 2, width), jnp.float32),
            pltpu.VMEM((2, 1, share), jnp.float32),
            pltpu.VMEM((TALL, WIDE, CORES, 1, n * share), jnp.float32),
            pltpu.VMEM((16, n * share), jnp.float32),
            pltpu.SemaphoreType.DMA((6,)),
            pltpu.SemaphoreType.DMA((3,)),
            pltpu.SemaphoreType.DMA((1,)),
            pltpu.SemaphoreType.DMA((1,)),
            pltpu.SemaphoreType.DMA((3, 19)),
            pltpu.SemaphoreType.DMA((1,)),
            pltpu.SemaphoreType.DMA((1,)),
            pltpu.SemaphoreType.DMA((TALL - 1,)),
            pltpu.SemaphoreType.DMA((2, TALL - 1)),
            pltpu.SemaphoreType.DMA((1,)),
            pltpu.SemaphoreType.DMA((1,)),
            pltpu.SemaphoreType.DMA((1,)),
            pltpu.SemaphoreType.DMA((1,)),
            pltpu.SemaphoreType.REGULAR,
        ],
        compiler_params=pltpu.CompilerParams(collective_id=0, has_side_effects=True, vmem_limit_bytes=32 * 2**20),
        name="gather",
    )(mix_share, *(pltpu.with_memory_space_constraint(w, pltpu.HBM) for w in held))
    serve_gate, serve_up, scale_gate, scale_up, serve_router = pl.pallas_call(
        place_kernel,
        out_shape=(
            jax.ShapeDtypeStruct((1, n * share, width), jnp.bfloat16),
            jax.ShapeDtypeStruct((1, n * share, width), jnp.bfloat16),
            jax.ShapeDtypeStruct((1, width), jnp.float32),
            jax.ShapeDtypeStruct((1, width), jnp.float32),
            jax.ShapeDtypeStruct((owners, n * share), jnp.bfloat16),
        ),
        in_specs=[in_vmem] * 3,
        out_specs=(in_hbm,) * 5,
        scratch_shapes=[pltpu.SemaphoreType.DMA((5,))],
        compiler_params=pltpu.CompilerParams(vmem_limit_bytes=32 * 2**20),
        name="place",
    )(gathered, scale, router)
    return (serve_gate, serve_up, scale_gate, scale_up, serve_router.T)


def solution(mesh):
    placed = (
        P("owner", "rows", None),
        P("owner", "rows", None),
        P("owner", "rows", None),
        P("owner", "rows", None),
        P("owner"),
        P("rows", "owner"),
        P("rows"),
    )
    return jax.shard_map(
        shards,
        mesh=mesh,
        in_specs=placed,
        out_specs=(
            P("owner", None, None),
            P("owner", None, None),
            P("owner", None),
            P("owner", None),
            P(),
        ),
        check_vma=False,
    )
```
